32 devices in a mesh: replica: 8 (over z, core), tp: 4 (over y, x).
Axes of the slice: x: 2, y: 2, z: 4, core: 2. Of those that a mesh axis runs over, the one named last changes fastest.
Arguments:
- token_ids: int32 [128], replicated, may hold values from 0 to 8191
- embed_table: bfloat16 [8192, 8192], P('replica', 'tp'), may hold values from -6 to 6
- norm_gain: bfloat16 [8192], replicated, may hold values from 0.099609375 to 1.8984375
- w_query: bfloat16 [8192, 4096], P(('replica', 'tp')), may hold values from -0.0625 to 0.0625
- w_keyvalue: bfloat16 [8192, 2, 512], P(('replica', 'tp')), may hold values from -0.0625 to 0.0625
- key_cache: bfloat16 [512, 1024, 128], P(('replica', 'tp')), may hold values from -360 to 360
- value_cache: bfloat16 [512, 1024, 128], P(('replica', 'tp')), may hold values from -6 to 6
- cache_lengths: int32 [128], P('replica'), may hold values from 1 to 1024, as said below
Outputs:
- context: bfloat16 [512, 1024], P(('replica', 'tp'))
- query_weight_tp: bfloat16 [8192, 4096], P(None, 'tp')
- keyvalue_weight_tp: bfloat16 [8192, 2, 512], P(None, None, 'tp')
The draws below stay inside these ranges and needn't reach their ends.
Inputs may be any that keep to these rules, and one draw needn't show every extreme that they name: `cache_lengths`: some sequence has exactly 1024 filled slots.
All inputs are finite; a program needn't handle non-finite values.
Results may differ from the reference program's by a relative error of at most 0.019.
The reference program's roundings to bfloat16 on the way count: a program that leaves them out, or rounds other values in their place, can miss the bound.
Values may be sent and summed in bfloat16 or wider, within the bound.
A program may use at most 128 MiB of HBM per device.

```python
import math
import jax
import jax.numpy as jnp
import numpy as np
from jax import lax

D = 8192
HD = 128
QHEADS = 32
KVHEADS = 4
BATCH = 16
CTX = 1024
VOCAB = 8192
GROUP = 8
SEQS = 128
CACHE_ROWS = 512
N_REPLICA = 8


def draw_key_cache(key, part):
    base = jnp.clip(jax.random.normal(key, (CACHE_ROWS, CTX, HD), jnp.float32), -6.0, 6.0)
    return base.astype(jnp.bfloat16)


def draw_cache_lengths(key, part):
    lengths = jax.random.randint(key, (SEQS,), 1, CTX + 1, jnp.int32)
    chosen = jax.random.randint(jax.random.fold_in(key, 3), (), 0, SEQS, jnp.int32)
    return jnp.where(jnp.arange(SEQS, dtype=jnp.int32) == chosen, CTX, lengths).astype(jnp.int32)


def plant(array, key, low, high):
    dims = array.shape
    spot = [jax.random.randint(jax.random.fold_in(key, axis), (), 0, dims[axis]) for axis in range(len(dims))]
    array = array.at[tuple(spot)].set(low)
    longest = dims.index(max(dims))
    spot[longest] = (spot[longest] + 1) % dims[longest]
    return array.at[tuple(spot)].set(high)


def level_of(stream_key, extent, pieces, least, largest):
    level = 1.0
    for dim, shards_of in pieces:
        heights = jax.random.uniform(jax.random.fold_in(jax.random.fold_in(stream_key, 6), dim), (shards_of,), jnp.float32, least / len(pieces), largest / len(pieces))
        level = level * jnp.repeat(jnp.exp(heights), extent[dim] // shards_of).reshape((-1,) + (1,) * (len(extent) - 1 - dim))
    return level


def rank_bounds(amount, skew):
    weights = [(1 << 20) // math.isqrt(grade ** skew) + 1 for grade in range(1, amount + 1)]
    spread = 1 + sum(weights) // (1 << 30)
    return np.cumsum(np.array([max(1, weight // spread) for weight in weights]))


def ranked(key, dims, number_of, skew):
    listing = rank_bounds(number_of, skew)
    ticket = jax.random.randint(jax.random.fold_in(key, 1), dims, 0, int(listing[number_of - 1]))
    grade = jnp.searchsorted(jnp.asarray(listing, jnp.int32), ticket, side="right")
    return jax.random.permutation(jax.random.fold_in(key, 2), number_of)[grade].astype(jnp.int32)


def normal_values(own_key, extent, width, limit, shards=(), held_as=jnp.bfloat16):
    gain = level_of(own_key, extent, shards, -0.22, 0.18) if shards else 1.0
    array = jax.random.normal(own_key, extent, jnp.float32) * width * gain
    return jnp.minimum(jnp.maximum(array, -limit), limit).astype(held_as)


def setup_inputs(seed: int = 0) -> dict:
    arg_keys = jax.random.split(jax.random.key(seed), 9)
    return {
        "token_ids": plant(ranked(arg_keys[0], (SEQS,), VOCAB, 2), jax.random.fold_in(arg_keys[0], 3), 0, VOCAB - 1).astype(jnp.int32),
        "embed_table": normal_values(arg_keys[1], (VOCAB, D), 1.0, 6.0, ((0, 8), (1, 4))),
        "norm_gain": jnp.clip(1.0 + 0.18 * jax.random.normal(arg_keys[2], (D,), jnp.float32), 0.099609375, 1.8984375).astype(jnp.bfloat16),
        "w_query": normal_values(arg_keys[3], (D, QHEADS * HD), D ** -0.5, 0.0625, ((0, 32),)),
        "w_keyvalue": normal_values(arg_keys[4], (D, 2, KVHEADS * HD), D ** -0.5, 0.0625, ((0, 32),)),
        "key_cache": draw_key_cache(jax.random.fold_in(arg_keys[8], 71), 0),
        "value_cache": normal_values(arg_keys[6], (CACHE_ROWS, CTX, HD), 1.0, 6.0, ((0, 32),)),
        "cache_lengths": draw_cache_lengths(jax.random.fold_in(arg_keys[8], 71), 0),
    }


def attend(query, keys, values, key_new, value_new, lengths):
    scale = query.shape[-1] ** (-0.5)
    scores = jnp.einsum('rgd,rcd->rgc', query.astype(jnp.float32), keys.astype(jnp.float32)) * scale
    position = lax.broadcasted_iota(jnp.int32, scores.shape, 2)
    scores = jnp.where(position < lengths[:, None, None], scores, -jnp.inf)
    own = jnp.einsum('rgd,rd->rg', query.astype(jnp.float32), key_new.astype(jnp.float32)) * scale
    top = jnp.maximum(lax.optimization_barrier(jnp.max(scores, axis=2)), own)
    weights = jnp.exp(scores - top[:, :, None])
    own_weight = jnp.exp(own - top)
    total = lax.optimization_barrier(jnp.sum(weights, axis=2)) + own_weight
    weights = (weights / total[:, :, None]).astype(jnp.bfloat16)
    own_weight = (own_weight / total).astype(jnp.bfloat16)
    context = jnp.einsum('rgc,rcd->rgd', weights.astype(jnp.float32), values.astype(jnp.float32))
    context = context + own_weight.astype(jnp.float32)[:, :, None] * value_new.astype(jnp.float32)[:, None, :]
    return context.astype(jnp.bfloat16)

def reference(token_ids, embed_table, norm_gain, w_query, w_keyvalue, key_cache, value_cache, cache_lengths):
    query_weight_tp = w_query
    keyvalue_weight_tp = w_keyvalue
    embedded = jnp.take(embed_table, token_ids, axis=0)
    values32 = embedded.astype(jnp.float32)
    mean_square = lax.optimization_barrier(jnp.mean(values32 * values32, axis=1, keepdims=True))
    normed = (values32 * lax.rsqrt(mean_square + 1e-05) * norm_gain.astype(jnp.float32)).astype(jnp.bfloat16)
    query = jnp.dot(normed, w_query, preferred_element_type=jnp.float32).astype(jnp.bfloat16)
    pair = jnp.dot(normed, w_keyvalue.reshape(D, 2 * KVHEADS * HD), preferred_element_type=jnp.float32).astype(jnp.bfloat16)
    pair = pair.reshape(SEQS, 2, KVHEADS * HD)
    query = query.reshape(N_REPLICA, BATCH, KVHEADS, GROUP, HD).transpose(0, 2, 1, 3, 4).reshape(N_REPLICA, KVHEADS * BATCH, GROUP, HD)
    key_new = pair[:, 0].reshape(N_REPLICA, BATCH, KVHEADS, HD).transpose(0, 2, 1, 3).reshape(N_REPLICA, KVHEADS * BATCH, HD)
    value_new = pair[:, 1].reshape(N_REPLICA, BATCH, KVHEADS, HD).transpose(0, 2, 1, 3).reshape(N_REPLICA, KVHEADS * BATCH, HD)
    keys = key_cache.reshape(N_REPLICA, KVHEADS * BATCH, CTX, HD)
    values = value_cache.reshape(N_REPLICA, KVHEADS * BATCH, CTX, HD)
    lengths = jnp.tile(cache_lengths.reshape(N_REPLICA, BATCH), (1, KVHEADS))

    def per_group(items):
        return attend(items[0], items[1], items[2], items[3], items[4], items[5])
    context = lax.map(per_group, (query, keys, values, key_new, value_new, lengths))
    context = context.reshape(CACHE_ROWS, GROUP * HD)
    return (context, query_weight_tp, keyvalue_weight_tp)
```

```python
import functools

import jax
import jax.numpy as jnp
from jax import lax
from jax.experimental import pallas as pl
from jax.experimental.pallas import tpu as pltpu
from jax.sharding import PartitionSpec as P


def attend(query, keys, values, key_new, value_new, lengths):
    scale = query.shape[-1] ** (-0.5)
    scores = jnp.einsum("rgd,rcd->rgc", query, keys, preferred_element_type=jnp.float32) * scale
    position = lax.broadcasted_iota(jnp.int32, scores.shape, 2)
    scores = jnp.where(position < lengths[:, None, None], scores, -jnp.inf)
    own = jnp.einsum("rgd,rd->rg", query, key_new, preferred_element_type=jnp.float32) * scale
    top = jnp.maximum(jnp.max(scores, axis=2), own)
    weights = jnp.exp(scores - top[:, :, None])
    own_weight = jnp.exp(own - top)
    total = jnp.sum(weights, axis=2) + own_weight
    weights = (weights / total[:, :, None]).astype(jnp.bfloat16)
    own_weight = (own_weight / total).astype(jnp.bfloat16)
    context = jnp.einsum("rgc,rcd->rgd", weights, values, preferred_element_type=jnp.float32)
    context = (
        context
        + own_weight.astype(jnp.float32)[:, :, None] * value_new.astype(jnp.float32)[:, None, :]
    )
    return context.astype(jnp.bfloat16)


def per_device(
    token_ids, embed_table, norm_gain, w_query, w_keyvalue, key_cache, value_cache, cache_lengths
):
    group_index = lax.axis_index("replica")
    tp_index = lax.axis_index("tp")
    vocab_rows, feature_cols = embed_table.shape
    batch = cache_lengths.shape[0]
    first_id = group_index * vocab_rows
    picked = token_ids - first_id
    columns = lax.broadcasted_iota(jnp.int32, (batch * lax.axis_size("replica"), vocab_rows), 1)
    onehot = (picked[:, None] == columns).astype(jnp.bfloat16)
    embedded = lax.psum_scatter(
        jnp.dot(onehot, embed_table, preferred_element_type=jnp.float32),
        "replica",
        scatter_dimension=0,
        tiled=True,
    ).astype(jnp.bfloat16)
    whole = lax.all_gather(embedded, "tp", axis=1, tiled=True)
    values32 = whole.astype(jnp.float32)
    mean_square = jnp.mean(values32 * values32, axis=1, keepdims=True)
    normed = (values32 * lax.rsqrt(mean_square + 1e-05) * norm_gain.astype(jnp.float32)).astype(
        jnp.bfloat16
    )
    width = normed.shape[1]
    query_rows = w_query.reshape(w_query.shape[0], 1, w_query.shape[1])
    query_mid, pair_mid = (
        lax.all_to_all(query_rows, "tp", split_axis=2, concat_axis=0, tiled=True),
        lax.all_to_all(w_keyvalue, "tp", split_axis=2, concat_axis=0, tiled=True),
    )
    flat_query = query_mid.reshape(query_mid.shape[0], query_mid.shape[2])
    pair_cols = pair_mid.shape[2]
    flat_pair = pair_mid.reshape(pair_mid.shape[0], 2 * pair_cols)
    query_full, pair_full = (
        lax.all_gather(flat_query, "replica", axis=0, tiled=True),
        lax.all_gather(flat_pair, "replica", axis=0, tiled=True),
    )
    query_acc = jnp.dot(normed, query_full, preferred_element_type=jnp.float32)
    pair_acc = jnp.dot(normed, pair_full, preferred_element_type=jnp.float32)
    query_local = query_acc.astype(jnp.bfloat16)
    pair_local = pair_acc.astype(jnp.bfloat16).reshape(batch, 2, pair_cols)
    query_heads, pair_heads = (
        lax.all_gather(query_local, "tp", axis=1, tiled=True),
        lax.all_gather(pair_local, "tp", axis=2, tiled=True),
    )
    head_size = key_cache.shape[2]
    kv_heads = pair_heads.shape[2] // head_size
    group = query_heads.shape[1] // (kv_heads * head_size)
    rows_here = key_cache.shape[0]
    first_row = tp_index * rows_here
    query_grouped = (
        query_heads.reshape(batch, kv_heads, group, head_size)
        .transpose(1, 0, 2, 3)
        .reshape(kv_heads * batch, group, head_size)
    )
    key_grouped = (
        pair_heads[:, 0]
        .reshape(batch, kv_heads, head_size)
        .transpose(1, 0, 2)
        .reshape(kv_heads * batch, head_size)
    )
    value_grouped = (
        pair_heads[:, 1]
        .reshape(batch, kv_heads, head_size)
        .transpose(1, 0, 2)
        .reshape(kv_heads * batch, head_size)
    )
    query_mine = lax.dynamic_slice_in_dim(query_grouped, first_row, rows_here, 0)
    key_mine = lax.dynamic_slice_in_dim(key_grouped, first_row, rows_here, 0)
    value_mine = lax.dynamic_slice_in_dim(value_grouped, first_row, rows_here, 0)
    sequence = (first_row + lax.broadcasted_iota(jnp.int32, (rows_here,), 0)) % batch
    matches = sequence[:, None] == lax.broadcasted_iota(jnp.int32, (rows_here, batch), 1)
    row_lengths = jnp.sum(jnp.where(matches, cache_lengths[None, :], 0), axis=1)
    context = attend(query_mine, key_cache, value_cache, key_mine, value_mine, row_lengths)
    context = context.reshape(rows_here, group * head_size)
    return (context, query_full, pair_full.reshape(width, 2, pair_cols))


MESH = pl.DeviceIdType.MESH


def exchange_kernel(
    planes,
    subs,
    token_in,
    gain_in,
    length_in,
    table_in,
    query_in,
    pair_in,
    key_in,
    value_in,
    query_out,
    pair_out,
    key_out,
    value_out,
    length_out,
    normed_ref,
    spread_ref,
    token_hold,
    gain_hold,
    gain_wide,
    length_hold,
    table_hold,
    onehot_ref,
    part_ref,
    given,
    joined,
    picked,
    relayed,
    relay_sum,
    relay_in,
    pieces,
    send_sem,
    recv_sem,
    across_sem,
    local_sem,
    give_send,
    give_recv,
    pick_send,
    pick_recv,
    relay_send,
    relay_recv,
    piece_send,
    piece_recv,
):
    r, t = lax.axis_index("replica"), lax.axis_index("tp")
    replicas = 2 * planes
    z, k = r // 2, lax.rem(r, 2)
    ty, tx = t // 2, lax.rem(t, 2)
    rows, query_cols = query_in.shape[0], query_out.shape[1]
    pair_cols = pair_out.shape[2]
    sub = rows // subs
    batch, feats = pieces.shape[1], pieces.shape[2]
    other = [t, ty * 2 + 1 - tx, (1 - ty) * 2 + tx, 3 - t]
    partner = z * 2 + 1 - k

    def piece_id(plane, core, tp):
        return (plane * 2 + core) * 4 + tp

    def part_of(ref, pid, s):
        return ref.at[pl.ds(pl.multiple_of(pid * rows + s * sub, sub), sub)]

    mine = piece_id(z, k, t)

    def columns(tp, first, count):
        return (
            query_in.at[
                pl.ds(first, count), pl.ds(pl.multiple_of(tp * query_cols, query_cols), query_cols)
            ],
            pair_in.at[
                pl.ds(first, count), :, pl.ds(pl.multiple_of(tp * pair_cols, pair_cols), pair_cols)
            ],
        )

    own = columns(t, 0, rows)
    where_own = pl.ds(pl.multiple_of(mine * rows, rows), rows)
    bring = [
        pltpu.make_async_copy(own[0], query_out.at[where_own], local_sem.at[0]),
        pltpu.make_async_copy(own[1], pair_out.at[where_own], local_sem.at[1]),
    ]
    fetch = [
        pltpu.make_async_copy(token_in, token_hold, local_sem.at[2]),
        pltpu.make_async_copy(table_in, table_hold, local_sem.at[3]),
        pltpu.make_async_copy(gain_in, gain_hold, local_sem.at[4]),
        pltpu.make_async_copy(length_in, length_hold, local_sem.at[5]),
        pltpu.make_async_copy(key_in, key_out, local_sem.at[6]),
        pltpu.make_async_copy(value_in, value_out, local_sem.at[7]),
    ]
    for copy in bring:
        copy.start()

    barrier = pltpu.get_barrier_semaphore()
    for j in range(1, 4):
        pl.semaphore_signal(barrier, inc=1, device_id=(r, other[j]), device_id_type=MESH)
    for step in range(1, replicas):
        pl.semaphore_signal(
            barrier, inc=1, device_id=(lax.rem(r + step, replicas), t), device_id_type=MESH
        )
    for copy in fetch[:2]:
        copy.start()
    pl.semaphore_wait(barrier, replicas - 1 + 3)

    def landed(pid, s):
        for c, out in enumerate((query_out, pair_out)):
            place = part_of(out, pid, s)
            pltpu.make_async_copy(place, place, recv_sem.at[c, pid * subs + s]).wait()

    def copies(pid, s, way, slot, target):
        return [
            pltpu.make_async_remote_copy(
                src_ref=part_of(out, pid, s),
                dst_ref=part_of(out, pid, s),
                send_sem=send_sem.at[c, way, slot * subs + s],
                recv_sem=recv_sem.at[c, pid * subs + s],
                device_id=target,
                device_id_type=MESH,
            )
            for c, out in enumerate((query_out, pair_out))
        ]

    def across(j, s):
        return [
            pltpu.make_async_remote_copy(
                src_ref=source,
                dst_ref=part_of(out, mine, s),
                send_sem=across_sem.at[c, (j - 1) * subs + s],
                recv_sem=recv_sem.at[c, mine * subs + s],
                device_id=(r, other[j]),
                device_id_type=MESH,
            )
            for c, (source, out) in enumerate(
                zip(
                    columns(other[j], pl.multiple_of(s * sub, sub), sub),
                    (query_out, pair_out),
                )
            )
        ]

    def onward(pid, s, slot, up, down, wait=False):
        def act(made):
            for copy in made:
                copy.wait_send() if wait else copy.start()

        if up:

            @pl.when(z < planes - 1)
            def _():
                act(copies(pid, s, 0, slot, (lax.rem(r + 2, replicas), t)))

        if down:

            @pl.when(z > 0)
            def _():
                act(copies(pid, s, 1, slot, (lax.rem(r + replicas - 2, replicas), t)))

        act(copies(pid, s, 2, slot, (partner, t)))

    def each_sub(act):
        def body(s, carry):
            act(s)
            return carry

        lax.fori_loop(0, subs, body, 0)

    def near(j, wait=False):
        pid = piece_id(z, k, other[j])

        def act(s):
            if not wait and j > 0:
                landed(pid, s)
            onward(pid, s, j, True, True, wait)

        each_sub(act)

    def far_away(far, j, wait=False):
        @pl.when(z >= far)
        def _():
            pid = piece_id(lax.rem(z + planes - far, planes), k, other[j])

            def act(s):
                if not wait:
                    landed(pid, s)
                onward(pid, s, 4 * far + j, True, False, wait)

            each_sub(act)

        @pl.when(z + far < planes)
        def _():
            pid = piece_id(lax.rem(z + far, planes), k, other[j])

            def act(s):
                if not wait:
                    landed(pid, s)
                onward(pid, s, 4 * (planes - 1 + far) + j, False, True, wait)

            each_sub(act)

    for copy in bring:
        copy.wait()

    def send_across(s):
        for j in range(1, 4):
            for copy in across(j, s):
                copy.start()

    near(0)
    each_sub(send_across)
    for copy in fetch[2:]:
        copy.start()

    gives = [
        pltpu.make_async_remote_copy(
            src_ref=part_ref.at[plane, 1 - k],
            dst_ref=given.at[plane],
            send_sem=give_send.at[plane],
            recv_sem=give_recv.at[plane],
            device_id=(partner, t),
            device_id_type=MESH,
        )
        for plane in range(planes)
    ]

    last = planes - 1

    def picks(dest, wait=None):
        stop = 1 if dest == 0 else last - 1 if dest == last else dest
        table, send, recv = (
            (picked, pick_send, pick_recv)
            if stop == dest
            else (relayed, relay_send, relay_recv)
        )

        @pl.when((z != dest) & (z != stop))
        def _():
            copy = pltpu.make_async_remote_copy(
                src_ref=joined.at[dest],
                dst_ref=table.at[z],
                send_sem=send.at[dest],
                recv_sem=recv.at[z],
                device_id=(stop * 2 + k, t),
                device_id_type=MESH,
            )
            copy.wait_send() if wait else copy.start()

    def arrived(table, recv, source):
        place = table.at[source]
        pltpu.make_async_copy(place, place, recv.at[source]).wait()

    def relay(dest):
        stop = 1 if dest == 0 else last - 1
        return pltpu.make_async_remote_copy(
            src_ref=relay_sum,
            dst_ref=relay_in,
            send_sem=relay_send.at[planes],
            recv_sem=relay_recv.at[planes],
            device_id=(dest * 2 + k, t),
            device_id_type=MESH,
        ), stop

    gather = [
        pltpu.make_async_remote_copy(
            src_ref=pieces.at[t],
            dst_ref=pieces.at[t],
            send_sem=piece_send.at[j - 1],
            recv_sem=piece_recv.at[j - 1],
            device_id=(r, other[j]),
            device_id_type=MESH,
        )
        for j in range(1, 4)
    ]

    def select_rows():
        fetch[0].wait()
        vocab_rows = table_hold.shape[0]
        tokens = token_hold.shape[1]
        lanes = 128
        wanted = jnp.broadcast_to(token_hold[...] - r * vocab_rows, (lanes, tokens)).T
        lane = lax.broadcasted_iota(jnp.int32, (tokens, lanes), 1)
        for first in range(0, vocab_rows, lanes):
            onehot_ref[:, first : first + lanes] = (wanted == lane + first).astype(
                onehot_ref.dtype
            )
        fetch[1].wait()
        block = 256

        def select(i, carry):
            where = pl.ds(pl.multiple_of(i * block, block), block)
            rows_here = jnp.dot(
                onehot_ref[...], table_hold[:, where], preferred_element_type=jnp.float32
            ).astype(jnp.bfloat16)
            part_ref[:, :, :, where] = rows_here.reshape(planes, 2, batch, block)
            return carry

        lax.fori_loop(0, feats // block, select, 0)

    def join():
        for copy in gives:
            copy.wait()
        for plane in range(planes):
            kept = part_ref[plane, k].astype(jnp.float32)
            joined[plane] = (kept + given[plane].astype(jnp.float32)).astype(jnp.bfloat16)

    def pass_on():
        for dest in (0, last):
            copy, stop = relay(dest)

            @pl.when(z == stop)
            def _():
                total = joined[dest].astype(jnp.float32)
                for source in range(planes):
                    if source not in (dest, stop):
                        arrived(relayed, relay_recv, source)
                        total = total + relayed[source].astype(jnp.float32)
                relay_sum[...] = total.astype(jnp.bfloat16)
                copy.start()

    def sum_picks():
        for dest in range(planes):

            @pl.when(z == dest)
            def _():
                total = joined[dest].astype(jnp.float32)
                if dest in (0, last):
                    relay(dest)[0].wait_recv()
                    total = total + relay_in[...].astype(jnp.float32)
                else:
                    for source in range(planes):
                        if source != dest:
                            arrived(picked, pick_recv, source)
                            total = total + picked[source].astype(jnp.float32)
                pieces[t] = total.astype(jnp.bfloat16)

    def normalise():
        fetch[2].wait()
        gain_wide[...] = gain_hold[...].astype(jnp.float32)
        for copy in gather:
            copy.wait()
        square = jnp.zeros((batch, 1), jnp.float32)
        for i in range(4):
            part = pieces[i].astype(jnp.float32)
            square = square + jnp.sum(part * part, axis=1, keepdims=True)
        factor = lax.rsqrt(square / (4 * feats) + 1e-05)
        lanes = gain_wide.shape[1]
        blocks = feats // lanes
        for i in range(4):

            def scaled(b, carry):
                part = pieces[i, :, pl.ds(pl.multiple_of(b * lanes, lanes), lanes)]
                gain = gain_wide[pl.ds(i * blocks + b, 1), :]
                where = pl.ds(pl.multiple_of(i * feats + b * lanes, lanes), lanes)
                normed_ref[:, where] = (part.astype(jnp.float32) * factor * gain).astype(
                    jnp.bfloat16
                )
                return carry

            lax.fori_loop(0, blocks, scaled, 0)
        block = 256
        line = lax.broadcasted_iota(jnp.int32, (block, 2 * block), 0)
        column = lax.broadcasted_iota(jnp.int32, (block, 2 * block), 1)
        even = (column == 2 * line).astype(jnp.bfloat16)
        odd = (column == 2 * line + 1).astype(jnp.bfloat16)

        def spread(i, carry):
            part = normed_ref[:, pl.ds(pl.multiple_of(i * block, block), block)]
            where = pl.ds(pl.multiple_of(i * 2 * block, 2 * block), 2 * block)
            spread_ref[0:batch, where] = jnp.dot(
                part, even, preferred_element_type=jnp.float32
            ).astype(jnp.bfloat16)
            spread_ref[batch : 2 * batch, where] = jnp.dot(
                part, odd, preferred_element_type=jnp.float32
            ).astype(jnp.bfloat16)
            return carry

        lax.fori_loop(0, 4 * feats // block, spread, 0)

    def lengths():
        fetch[3].wait()
        group = length_out.shape[1]
        for s in range(batch):
            length_out[s] = jnp.full((group, length_out.shape[2]), length_hold[s], jnp.int32)

    select_rows()
    for copy in gives:
        copy.start()
    join()
    for dest in range(planes):
        picks(dest)
    near(1)
    near(2)
    far_away(1, 0)
    near(3)
    pass_on()
    far_away(1, 1)
    far_away(1, 2)
    sum_picks()
    for copy in gather:
        copy.start()
    far_away(1, 3)
    normalise()
    lengths()
    for far in range(2, planes):
        for j in range(4):
            far_away(far, j)

    for copy in fetch[4:]:
        copy.wait()

    def sent_across(s):
        for j in range(1, 4):
            for copy in across(j, s):
                copy.wait_send()

    each_sub(sent_across)
    for dest in range(planes):
        picks(dest, wait=True)
    for dest in (0, last):
        copy, stop = relay(dest)

        @pl.when(z == stop)
        def _():
            copy.wait_send()

    for j in range(4):
        near(j, wait=True)
    for far in range(1, planes):
        for j in range(4):
            far_away(far, j, wait=True)
    for plane in range(planes):
        for j in range(4):
            pid = piece_id(plane, 1 - k, j)
            each_sub(functools.partial(landed, pid))


def exchange(
    token_ids, norm_gain, embed_table, w_query, w_keyvalue, key_cache, value_cache, lengths, planes
):
    rows, all_query = w_query.shape
    query_cols, pair_cols = all_query // 4, w_keyvalue.shape[2] // 4
    replicas = 2 * planes
    width = rows * replicas * 4
    feats = embed_table.shape[1]
    kind = w_query.dtype
    batch, head_size = lengths.shape[0], key_cache.shape[2]
    group = query_cols // head_size
    tokens = token_ids.shape[0]
    lanes = 128
    subs = 2
    anywhere = pl.BlockSpec(memory_space=pl.ANY)
    vmem = pl.BlockSpec(memory_space=pltpu.VMEM)
    dma = pltpu.SemaphoreType.DMA
    slots = 4 * (2 * planes - 1) * subs
    shape = jax.ShapeDtypeStruct
    return pl.pallas_call(
        functools.partial(exchange_kernel, planes, subs),
        out_shape=(
            pltpu.VMEM((width, query_cols), kind),
            pltpu.VMEM((width, 2, pair_cols), kind),
            pltpu.VMEM(key_cache.shape, kind),
            pltpu.VMEM(value_cache.shape, kind),
            pltpu.VMEM((batch, group, head_size), jnp.int32),
            pltpu.VMEM((batch, width), kind),
            pltpu.VMEM((2 * batch, 2 * width), kind),
        ),
        in_specs=[anywhere] * 8,
        out_specs=(vmem,) * 7,
        scratch_shapes=[
            pltpu.VMEM((1, tokens), jnp.int32),
            pltpu.VMEM((width // lanes, lanes), kind),
            pltpu.VMEM((width // lanes, lanes), jnp.float32),
            pltpu.SMEM((batch,), jnp.int32),
            pltpu.VMEM(embed_table.shape, kind),
            pltpu.VMEM((tokens, embed_table.shape[0]), kind),
            pltpu.VMEM((planes, 2, batch, feats), kind),
            pltpu.VMEM((planes, batch, feats), kind),
            pltpu.VMEM((planes, batch, feats), kind),
            pltpu.VMEM((planes, batch, feats), kind),
            pltpu.VMEM((planes, batch, feats), kind),
            pltpu.VMEM((batch, feats), kind),
            pltpu.VMEM((batch, feats), kind),
            pltpu.VMEM((4, batch, feats), kind),
            dma((2, 3, slots)),
            dma((2, replicas * 4 * subs)),
            dma((2, 3 * subs)),
            dma((8,)),
            dma((planes,)),
            dma((planes,)),
            dma((planes,)),
            dma((planes,)),
            dma((planes + 1,)),
            dma((planes + 1,)),
            dma((3,)),
            dma((3,)),
        ],
        compiler_params=pltpu.CompilerParams(
            collective_id=0, has_side_effects=True, vmem_limit_bytes=8 * 2**20
        ),
        cost_estimate=pl.CostEstimate(
            flops=2 * 10**11, bytes_accessed=2 * width * query_cols, transcendentals=0
        ),
        name="weight_exchange",
    )(
        *(
            pltpu.with_memory_space_constraint(operand, pltpu.HBM)
            for operand in (
                token_ids.reshape(1, tokens),
                norm_gain.reshape(-1, lanes),
                lengths,
                embed_table,
                w_query,
                w_keyvalue,
                key_cache,
                value_cache,
            )
        )
    )


def finish_kernel(
    normed_ref,
    spread_ref,
    query_all,
    pair_all,
    key_ref,
    value_ref,
    length_ref,
    query_ref,
    pair_ref,
    context_ref,
    query_heads,
    context_heads,
    sems,
):
    batch, width = normed_ref.shape
    query_cols, pair_cols = query_all.shape[1], pair_all.shape[1]
    group, head_size = query_heads.shape[1], query_heads.shape[2]
    parts = sems.shape[1]
    stores = []
    for c, (held, out) in enumerate(((query_all, query_ref), (pair_all, pair_ref))):
        size = held.shape[0] // parts
        for i in range(parts):
            where = pl.ds(i * size, size)
            stores.append(pltpu.make_async_copy(held.at[where], out.at[where], sems.at[c, i]))
    for copy in stores:
        copy.start()

    block = 512

    def project(i, carry):
        query, pair = carry
        here = pl.ds(pl.multiple_of(i * block, block), block)
        twice = pl.ds(pl.multiple_of(i * 2 * block, 2 * block), 2 * block)
        query = query + jnp.dot(
            normed_ref[:, here], query_all[here, :], preferred_element_type=jnp.float32
        )
        pair = pair + jnp.dot(
            spread_ref[:, twice], pair_all[twice, :], preferred_element_type=jnp.float32
        )
        return query, pair

    query, pair = lax.fori_loop(
        0,
        width // block,
        project,
        (
            jnp.zeros((batch, query_cols), jnp.float32),
            jnp.zeros((2 * batch, pair_cols), jnp.float32),
        ),
    )
    query = query.astype(jnp.bfloat16).astype(jnp.float32)
    pair = pair.astype(jnp.bfloat16).astype(jnp.float32)
    for j in range(group):
        query_heads[:, j, :] = query[:, j * head_size : (j + 1) * head_size]

    scale = head_size ** (-0.5)
    slots = key_ref.shape[1]
    position = lax.broadcasted_iota(jnp.int32, (group, slots), 1)
    for s in range(batch):
        heads = query_heads[s]
        scores = (
            lax.dot_general(
                heads.astype(jnp.bfloat16),
                key_ref[s],
                (((1,), (1,)), ((), ())),
                preferred_element_type=jnp.float32,
            )
            * scale
        )
        scores = jnp.where(position < length_ref[s, :, 0:1], scores, -jnp.inf)
        own = jnp.sum(heads * pair[s : s + 1], axis=1, keepdims=True) * scale
        top = jnp.maximum(jnp.max(scores, axis=1, keepdims=True), own)
        weights = jnp.exp(scores - top)
        own_weight = jnp.exp(own - top)
        total = jnp.sum(weights, axis=1, keepdims=True) + own_weight
        weights = (weights / total).astype(jnp.bfloat16)
        own_weight = (own_weight / total).astype(jnp.bfloat16).astype(jnp.float32)
        context = jnp.dot(weights, value_ref[s], preferred_element_type=jnp.float32)
        context_heads[s] = context + own_weight * pair[batch + s : batch + s + 1]
    for j in range(group):
        context_ref[:, j * head_size : (j + 1) * head_size] = context_heads[:, j, :].astype(
            context_ref.dtype
        )
    for copy in stores:
        copy.wait()


def finish(normed, spread, query_all, pair_all, keys, values, lengths):
    batch, width = normed.shape
    query_cols, pair_cols = query_all.shape[1], pair_all.shape[2]
    head_size = keys.shape[2]
    group = query_cols // head_size
    pair_flat = pair_all.reshape(2 * width, pair_cols)
    anywhere = pl.BlockSpec(memory_space=pl.ANY)
    vmem = pl.BlockSpec(memory_space=pltpu.VMEM)
    shape = jax.ShapeDtypeStruct
    query_out, pair_out, context = pl.pallas_call(
        finish_kernel,
        out_shape=(
            shape(query_all.shape, query_all.dtype),
            shape(pair_flat.shape, pair_all.dtype),
            shape((batch, query_cols), normed.dtype),
        ),
        in_specs=[vmem] * 7,
        out_specs=(
            pl.BlockSpec(memory_space=pltpu.HBM),
            pl.BlockSpec(memory_space=pltpu.HBM),
            vmem,
        ),
        scratch_shapes=[
            pltpu.VMEM((batch, group, head_size), jnp.float32),
            pltpu.VMEM((batch, group, head_size), jnp.float32),
            pltpu.SemaphoreType.DMA((2, 4)),
        ],
        compiler_params=pltpu.CompilerParams(vmem_limit_bytes=8 * 2**20),
        cost_estimate=pl.CostEstimate(
            flops=2 * batch * width * (query_cols + 4 * pair_cols),
            bytes_accessed=4 * width * (query_cols + 2 * pair_cols),
            transcendentals=0,
        ),
        name="project_attend_store",
    )(normed, spread, query_all, pair_flat, keys, values, lengths)
    return context, query_out, pair_out.reshape(width, 2, pair_cols)


def per_device_line(
    planes,
    token_ids,
    embed_table,
    norm_gain,
    w_query,
    w_keyvalue,
    key_cache,
    value_cache,
    cache_lengths,
):
    query_all, pair_all, keys, values, lengths, normed, spread = exchange(
        token_ids,
        norm_gain,
        embed_table,
        w_query,
        w_keyvalue,
        key_cache,
        value_cache,
        cache_lengths,
        planes,
    )
    return finish(normed, spread, query_all, pair_all, keys, values, lengths)


def solution(mesh):
    replicas, tp = mesh.shape["replica"], mesh.shape["tp"]

    def body(*args):
        key_cache, lengths, w_keyvalue = args[5], args[7], args[4]
        one_head = w_keyvalue.shape[2] == tp * key_cache.shape[2]
        own_rows = key_cache.shape[0] == lengths.shape[0]
        if tp == 4 and replicas % 2 == 0 and replicas > 6 and one_head and own_rows:
            return per_device_line(replicas // 2, *args)
        return per_device(*args)

    return jax.shard_map(
        body,
        mesh=mesh,
        in_specs=(
            P(),
            P("replica", "tp"),
            P(),
            P(("replica", "tp"), None),
            P(("replica", "tp"), None, None),
            P(("replica", "tp"), None, None),
            P(("replica", "tp"), None, None),
            P("replica"),
        ),
        out_specs=(P(("replica", "tp"), None), P(None, "tp"), P(None, None, "tp")),
        check_vma=False,
    )
```

```python
import functools

import jax
import jax.numpy as jnp
from jax import lax
from jax.experimental import pallas as pl
from jax.experimental.pallas import tpu as pltpu
from jax.sharding import PartitionSpec as P


def attend(query, keys, values, key_new, value_new, lengths):
    scale = query.shape[-1] ** (-0.5)
    scores = jnp.einsum("rgd,rcd->rgc", query, keys, preferred_element_type=jnp.float32) * scale
    position = lax.broadcasted_iota(jnp.int32, scores.shape, 2)
    scores = jnp.where(position < lengths[:, None, None], scores, -jnp.inf)
    own = jnp.einsum("rgd,rd->rg", query, key_new, preferred_element_type=jnp.float32) * scale
    top = jnp.maximum(jnp.max(scores, axis=2), own)
    weights = jnp.exp(scores - top[:, :, None])
    own_weight = jnp.exp(own - top)
    total = jnp.sum(weights, axis=2) + own_weight
    weights = (weights / total[:, :, None]).astype(jnp.bfloat16)
    own_weight = (own_weight / total).astype(jnp.bfloat16)
    context = jnp.einsum("rgc,rcd->rgd", weights, values, preferred_element_type=jnp.float32)
    context = (
        context
        + own_weight.astype(jnp.float32)[:, :, None] * value_new.astype(jnp.float32)[:, None, :]
    )
    return context.astype(jnp.bfloat16)


def per_device(
    token_ids, embed_table, norm_gain, w_query, w_keyvalue, key_cache, value_cache, cache_lengths
):
    group_index = lax.axis_index("replica")
    tp_index = lax.axis_index("tp")
    vocab_rows, feature_cols = embed_table.shape
    batch = cache_lengths.shape[0]
    first_id = group_index * vocab_rows
    picked = token_ids - first_id
    columns = lax.broadcasted_iota(jnp.int32, (batch * lax.axis_size("replica"), vocab_rows), 1)
    onehot = (picked[:, None] == columns).astype(jnp.bfloat16)
    embedded = lax.psum_scatter(
        jnp.dot(onehot, embed_table, preferred_element_type=jnp.float32),
        "replica",
        scatter_dimension=0,
        tiled=True,
    ).astype(jnp.bfloat16)
    whole = lax.all_gather(embedded, "tp", axis=1, tiled=True)
    values32 = whole.astype(jnp.float32)
    mean_square = jnp.mean(values32 * values32, axis=1, keepdims=True)
    normed = (values32 * lax.rsqrt(mean_square + 1e-05) * norm_gain.astype(jnp.float32)).astype(
        jnp.bfloat16
    )
    width = normed.shape[1]
    query_rows = w_query.reshape(w_query.shape[0], 1, w_query.shape[1])
    query_mid, pair_mid = (
        lax.all_to_all(query_rows, "tp", split_axis=2, concat_axis=0, tiled=True),
        lax.all_to_all(w_keyvalue, "tp", split_axis=2, concat_axis=0, tiled=True),
    )
    flat_query = query_mid.reshape(query_mid.shape[0], query_mid.shape[2])
    pair_cols = pair_mid.shape[2]
    flat_pair = pair_mid.reshape(pair_mid.shape[0], 2 * pair_cols)
    query_full, pair_full = (
        lax.all_gather(flat_query, "replica", axis=0, tiled=True),
        lax.all_gather(flat_pair, "replica", axis=0, tiled=True),
    )
    query_acc = jnp.dot(normed, query_full, preferred_element_type=jnp.float32)
    pair_acc = jnp.dot(normed, pair_full, preferred_element_type=jnp.float32)
    query_local = query_acc.astype(jnp.bfloat16)
    pair_local = pair_acc.astype(jnp.bfloat16).reshape(batch, 2, pair_cols)
    query_heads, pair_heads = (
        lax.all_gather(query_local, "tp", axis=1, tiled=True),
        lax.all_gather(pair_local, "tp", axis=2, tiled=True),
    )
    head_size = key_cache.shape[2]
    kv_heads = pair_heads.shape[2] // head_size
    group = query_heads.shape[1] // (kv_heads * head_size)
    rows_here = key_cache.shape[0]
    first_row = tp_index * rows_here
    query_grouped = (
        query_heads.reshape(batch, kv_heads, group, head_size)
        .transpose(1, 0, 2, 3)
        .reshape(kv_heads * batch, group, head_size)
    )
    key_grouped = (
        pair_heads[:, 0]
        .reshape(batch, kv_heads, head_size)
        .transpose(1, 0, 2)
        .reshape(kv_heads * batch, head_size)
    )
    value_grouped = (
        pair_heads[:, 1]
        .reshape(batch, kv_heads, head_size)
        .transpose(1, 0, 2)
        .reshape(kv_heads * batch, head_size)
    )
    query_mine = lax.dynamic_slice_in_dim(query_grouped, first_row, rows_here, 0)
    key_mine = lax.dynamic_slice_in_dim(key_grouped, first_row, rows_here, 0)
    value_mine = lax.dynamic_slice_in_dim(value_grouped, first_row, rows_here, 0)
    sequence = (first_row + lax.broadcasted_iota(jnp.int32, (rows_here,), 0)) % batch
    matches = sequence[:, None] == lax.broadcasted_iota(jnp.int32, (rows_here, batch), 1)
    row_lengths = jnp.sum(jnp.where(matches, cache_lengths[None, :], 0), axis=1)
    context = attend(query_mine, key_cache, value_cache, key_mine, value_mine, row_lengths)
    context = context.reshape(rows_here, group * head_size)
    return (context, query_full, pair_full.reshape(width, 2, pair_cols))


MESH = pl.DeviceIdType.MESH


def exchange_kernel(
    planes,
    subs,
    token_in,
    gain_in,
    length_in,
    table_in,
    query_in,
    pair_in,
    key_in,
    value_in,
    query_out,
    pair_out,
    key_out,
    value_out,
    length_out,
    normed_ref,
    spread_ref,
    query_acc,
    token_hold,
    gain_hold,
    gain_wide,
    length_hold,
    table_hold,
    onehot_ref,
    part_ref,
    given,
    joined,
    sums,
    brought,
    pieces,
    send_sem,
    recv_sem,
    hand_recv,
    across_sem,
    local_sem,
    give_send,
    give_recv,
    sum_send,
    sum_recv,
    piece_send,
    piece_recv,
):
    r, t = lax.axis_index("replica"), lax.axis_index("tp")
    replicas = 2 * planes
    z, k = r // 2, lax.rem(r, 2)
    ty, tx = t // 2, lax.rem(t, 2)
    rows, query_cols = query_in.shape[0], query_out.shape[1]
    pair_cols = pair_out.shape[2]
    sub = rows // subs
    batch, feats = pieces.shape[1], pieces.shape[2]
    other = [t, ty * 2 + 1 - tx, (1 - ty) * 2 + tx, 3 - t]
    partner = z * 2 + 1 - k

    def piece_id(plane, core, tp):
        return (plane * 2 + core) * 4 + tp

    def part_of(ref, pid, s):
        return ref.at[pl.ds(pl.multiple_of(pid * rows + s * sub, sub), sub)]

    mine = piece_id(z, k, t)

    def columns(tp, first, count):
        return (
            query_in.at[
                pl.ds(first, count), pl.ds(pl.multiple_of(tp * query_cols, query_cols), query_cols)
            ],
            pair_in.at[
                pl.ds(first, count), :, pl.ds(pl.multiple_of(tp * pair_cols, pair_cols), pair_cols)
            ],
        )

    own = columns(t, 0, rows)
    where_own = pl.ds(pl.multiple_of(mine * rows, rows), rows)
    bring = [
        pltpu.make_async_copy(own[0], query_out.at[where_own], local_sem.at[0]),
        pltpu.make_async_copy(own[1], pair_out.at[where_own], local_sem.at[1]),
    ]
    fetch = [
        pltpu.make_async_copy(token_in, token_hold, local_sem.at[2]),
        pltpu.make_async_copy(table_in, table_hold, local_sem.at[3]),
        pltpu.make_async_copy(gain_in, gain_hold, local_sem.at[4]),
        pltpu.make_async_copy(length_in, length_hold, local_sem.at[5]),
        pltpu.make_async_copy(key_in, key_out, local_sem.at[6]),
        pltpu.make_async_copy(value_in, value_out, local_sem.at[7]),
    ]
    for copy in bring:
        copy.start()

    barrier = pltpu.get_barrier_semaphore()
    for j in range(1, 4):
        pl.semaphore_signal(barrier, inc=1, device_id=(r, other[j]), device_id_type=MESH)
    pl.semaphore_signal(barrier, inc=1, device_id=(partner, t), device_id_type=MESH)
    above, below = lax.rem(r + 2, replicas), lax.rem(r + replicas - 2, replicas)

    @pl.when(z < planes - 1)
    def _():
        pl.semaphore_signal(barrier, inc=1, device_id=(above, t), device_id_type=MESH)

    @pl.when(z > 0)
    def _():
        pl.semaphore_signal(barrier, inc=1, device_id=(below, t), device_id_type=MESH)

    for copy in fetch[:2]:
        copy.start()
    pl.semaphore_wait(barrier, 4 + jnp.minimum(z, 1) + jnp.minimum(planes - 1 - z, 1))

    def landed(pid, s):
        for c, out in enumerate((query_out, pair_out)):
            place = part_of(out, pid, s)
            pltpu.make_async_copy(place, place, recv_sem.at[c, pid * subs + s]).wait()

    def send(pid, s, way, target):
        for c, out in enumerate((query_out, pair_out)):
            pltpu.make_async_remote_copy(
                src_ref=part_of(out, pid, s),
                dst_ref=part_of(out, pid, s),
                send_sem=send_sem.at[c, way],
                recv_sem=hand_recv.at[c, pid] if way == 2 else recv_sem.at[c, pid * subs + s],
                device_id=target,
                device_id_type=MESH,
            ).start()

    def sent(way, pieces_sent):
        for c, out in enumerate((query_out, pair_out)):
            place = out.at[0 : pieces_sent * rows]
            pltpu.make_async_copy(place, place, send_sem.at[c, way]).wait()

    def handed(pid):
        for c, out in enumerate((query_out, pair_out)):
            place = out.at[pl.ds(pl.multiple_of(pid * rows, rows), rows)]
            pltpu.make_async_copy(place, place, hand_recv.at[c, pid]).wait()

    def across(j, s):
        return [
            pltpu.make_async_remote_copy(
                src_ref=source,
                dst_ref=part_of(out, mine, s),
                send_sem=across_sem.at[c],
                recv_sem=recv_sem.at[c, mine * subs + s],
                device_id=(r, other[j]),
                device_id_type=MESH,
            )
            for c, (source, out) in enumerate(
                zip(
                    columns(other[j], pl.multiple_of(s * sub, sub), sub),
                    (query_out, pair_out),
                )
            )
        ]

    def onward(pid, s, up, down):
        if up:

            @pl.when(z < planes - 1)
            def _():
                send(pid, s, 0, (above, t))

        if down:

            @pl.when(z > 0)
            def _():
                send(pid, s, 1, (below, t))

        send(pid, s, 2, (partner, t))

    def each_sub(act):
        def body(s, carry):
            act(s)
            return carry

        lax.fori_loop(0, subs, body, 0)

    def near(j):
        pid = piece_id(z, k, other[j])

        def act(s):
            if j > 0:
                landed(pid, s)
            onward(pid, s, True, True)

        each_sub(act)

    def planes_at(far, act):
        if far == 0:
            act(z, True)
            return

        @pl.when(z >= far)
        def _():
            act(lax.rem(z + planes - far, planes), True)

        @pl.when(z + far < planes)
        def _():
            act(lax.rem(z + far, planes), False)

    def far_away(far, j):
        def forward(plane, up):
            pid = piece_id(plane, k, other[j])

            def act(s):
                landed(pid, s)
                onward(pid, s, up, not up)

            each_sub(act)

        planes_at(far, forward)

    def multiply(far, j):
        def both(plane, up):
            handed(piece_id(plane, 1 - k, other[j]))

            def add(core, carry):
                pid = piece_id(plane, core, other[j])
                where = pl.ds(pl.multiple_of(pid * rows, rows), rows)
                query_acc[...] += jnp.dot(
                    normed_ref[:, where], query_out[where, :], preferred_element_type=jnp.float32
                )
                return carry

            lax.fori_loop(0, 2, add, 0)

        planes_at(far, both)

    for copy in bring:
        copy.wait()

    def send_across(j):
        def act(s):
            for copy in across(j, s):
                copy.start()

        each_sub(act)

    near(0)
    for j in range(1, 4):
        send_across(j)
    for copy in fetch[2:]:
        copy.start()

    gives = [
        pltpu.make_async_remote_copy(
            src_ref=part_ref.at[plane, 1 - k],
            dst_ref=given.at[plane],
            send_sem=give_send.at[plane],
            recv_sem=give_recv.at[plane],
            device_id=(partner, t),
            device_id_type=MESH,
        )
        for plane in range(planes)
    ]

    last = planes - 1

    def passing(hop, wait=False):
        for way in range(2):
            for plane in range(planes - 1):
                if plane != hop and not wait:
                    continue
                place = plane if way == 0 else last - plane
                target = (place + 1 if way == 0 else place - 1) * 2 + k
                dests = range(place + 1, planes) if way == 0 else range(place)

                @pl.when(z == place)
                def _():
                    for dest in dests:
                        if plane > 0 and not wait:
                            came(way, dest)
                            total = joined[dest].astype(jnp.float32) + brought[
                                way, dest
                            ].astype(jnp.float32)
                            sums[way, dest] = total.astype(jnp.bfloat16)
                        copy = pltpu.make_async_remote_copy(
                            src_ref=sums.at[way, dest] if plane > 0 else joined.at[dest],
                            dst_ref=brought.at[way, dest],
                            send_sem=sum_send.at[way, dest],
                            recv_sem=sum_recv.at[way, dest],
                            device_id=(target, t),
                            device_id_type=MESH,
                        )
                        copy.wait_send() if wait else copy.start()

    def came(way, dest):
        place = brought.at[way, dest]
        pltpu.make_async_copy(place, place, sum_recv.at[way, dest]).wait()

    gather = [
        pltpu.make_async_remote_copy(
            src_ref=pieces.at[t],
            dst_ref=pieces.at[t],
            send_sem=piece_send.at[j - 1],
            recv_sem=piece_recv.at[j - 1],
            device_id=(r, other[j]),
            device_id_type=MESH,
        )
        for j in range(1, 4)
    ]

    def select_rows():
        fetch[0].wait()
        vocab_rows = table_hold.shape[0]
        tokens = token_hold.shape[1]
        lanes = 128
        wanted = jnp.broadcast_to(token_hold[...] - r * vocab_rows, (lanes, tokens)).T
        lane = lax.broadcasted_iota(jnp.int32, (tokens, lanes), 1)
        for first in range(0, vocab_rows, lanes):
            onehot_ref[:, first : first + lanes] = (wanted == lane + first).astype(
                onehot_ref.dtype
            )
        fetch[1].wait()
        block = 256

        def select(i, carry):
            where = pl.ds(pl.multiple_of(i * block, block), block)
            rows_here = jnp.dot(
                onehot_ref[...], table_hold[:, where], preferred_element_type=jnp.float32
            ).astype(jnp.bfloat16)
            part_ref[:, :, :, where] = rows_here.reshape(planes, 2, batch, block)
            return carry

        lax.fori_loop(0, feats // block, select, 0)

    def join():
        for copy in gives:
            copy.wait()
        for plane in range(planes):
            kept = part_ref[plane, k].astype(jnp.float32)
            joined[plane] = (kept + given[plane].astype(jnp.float32)).astype(jnp.bfloat16)

    def sum_all():
        for dest in range(planes):

            @pl.when(z == dest)
            def _():
                total = joined[dest].astype(jnp.float32)
                for way in range(2):
                    if dest != (0 if way == 0 else last):
                        came(way, dest)
                        total = total + brought[way, dest].astype(jnp.float32)
                pieces[t] = total.astype(jnp.bfloat16)

    def normalise():
        fetch[2].wait()
        gain_wide[...] = gain_hold[...].astype(jnp.float32)
        for copy in gather:
            copy.wait()
        square = jnp.zeros((batch, 1), jnp.float32)
        for i in range(4):
            part = pieces[i].astype(jnp.float32)
            square = square + jnp.sum(part * part, axis=1, keepdims=True)
        factor = lax.rsqrt(square / (4 * feats) + 1e-05)
        lanes = gain_wide.shape[1]
        blocks = feats // lanes
        for i in range(4):

            def scaled(b, carry):
                part = pieces[i, :, pl.ds(pl.multiple_of(b * lanes, lanes), lanes)]
                gain = gain_wide[pl.ds(i * blocks + b, 1), :]
                where = pl.ds(pl.multiple_of(i * feats + b * lanes, lanes), lanes)
                normed_ref[:, where] = (part.astype(jnp.float32) * factor * gain).astype(
                    jnp.bfloat16
                )
                return carry

            lax.fori_loop(0, blocks, scaled, 0)
        block = 256
        line = lax.broadcasted_iota(jnp.int32, (block, 2 * block), 0)
        column = lax.broadcasted_iota(jnp.int32, (block, 2 * block), 1)
        even = (column == 2 * line).astype(jnp.bfloat16)
        odd = (column == 2 * line + 1).astype(jnp.bfloat16)

        def spread(i, carry):
            part = normed_ref[:, pl.ds(pl.multiple_of(i * block, block), block)]
            where = pl.ds(pl.multiple_of(i * 2 * block, 2 * block), 2 * block)
            spread_ref[0:batch, where] = jnp.dot(
                part, even, preferred_element_type=jnp.float32
            ).astype(jnp.bfloat16)
            spread_ref[batch : 2 * batch, where] = jnp.dot(
                part, odd, preferred_element_type=jnp.float32
            ).astype(jnp.bfloat16)
            return carry

        lax.fori_loop(0, 4 * feats // block, spread, 0)

    def lengths():
        fetch[3].wait()
        group = length_out.shape[1]
        for s in range(batch):
            length_out[s] = jnp.full((group, length_out.shape[2]), length_hold[s], jnp.int32)

    select_rows()
    for copy in gives:
        copy.start()
    join()
    passing(0)
    order = [(0, 1), (0, 2), (1, 0), (0, 3)]
    order += [(far, j) for far in range(1, planes) for j in range(4) if (far, j) != (1, 0)]
    middle = len(order) - 5
    for step, (far, j) in enumerate(order):
        near(j) if far == 0 else far_away(far, j)
        if step == 1:
            passing(1)
        if step > 4 and step - 3 < planes - 1:
            passing(step - 3)
        if step == middle - 1:
            sum_all()
            for copy in gather:
                copy.start()
        if step == middle:
            normalise()
            lengths()
            query_acc[...] = jnp.zeros_like(query_acc)
            for past in [(0, 0)] + order[:middle]:
                multiply(*past)
        if step > middle:
            multiply(*order[step - 1])

    for copy in fetch[4:]:
        copy.wait()
    for c, out in enumerate((query_out, pair_out)):
        place = out.at[0 : 3 * rows]
        pltpu.make_async_copy(place, place, across_sem.at[c]).wait()
    passing(0, wait=True)
    multiply(*order[-1])
    for place in range(planes):

        @pl.when(z == place)
        def _():
            if place < last:
                sent(0, 4 * (place + 1))
            if place > 0:
                sent(1, 4 * (planes - place))

    sent(2, 4 * planes)


def exchange(
    token_ids, norm_gain, embed_table, w_query, w_keyvalue, key_cache, value_cache, lengths, planes
):
    rows, all_query = w_query.shape
    query_cols, pair_cols = all_query // 4, w_keyvalue.shape[2] // 4
    replicas = 2 * planes
    width = rows * replicas * 4
    feats = embed_table.shape[1]
    kind = w_query.dtype
    batch, head_size = lengths.shape[0], key_cache.shape[2]
    group = query_cols // head_size
    tokens = token_ids.shape[0]
    lanes = 128
    subs = 2
    anywhere = pl.BlockSpec(memory_space=pl.ANY)
    vmem = pl.BlockSpec(memory_space=pltpu.VMEM)
    dma = pltpu.SemaphoreType.DMA
    shape = jax.ShapeDtypeStruct
    return pl.pallas_call(
        functools.partial(exchange_kernel, planes, subs),
        out_shape=(
            pltpu.VMEM((width, query_cols), kind),
            pltpu.VMEM((width, 2, pair_cols), kind),
            pltpu.VMEM(key_cache.shape, kind),
            pltpu.VMEM(value_cache.shape, kind),
            pltpu.VMEM((batch, group, head_size), jnp.int32),
            pltpu.VMEM((batch, width), kind),
            pltpu.VMEM((2 * batch, 2 * width), kind),
            pltpu.VMEM((batch, query_cols), jnp.float32),
        ),
        in_specs=[anywhere] * 8,
        out_specs=(vmem,) * 8,
        scratch_shapes=[
            pltpu.VMEM((1, tokens), jnp.int32),
            pltpu.VMEM((width // lanes, lanes), kind),
            pltpu.VMEM((width // lanes, lanes), jnp.float32),
            pltpu.SMEM((batch,), jnp.int32),
            pltpu.VMEM(embed_table.shape, kind),
            pltpu.VMEM((tokens, embed_table.shape[0]), kind),
            pltpu.VMEM((planes, 2, batch, feats), kind),
            pltpu.VMEM((planes, batch, feats), kind),
            pltpu.VMEM((planes, batch, feats), kind),
            pltpu.VMEM((2, planes, batch, feats), kind),
            pltpu.VMEM((2, planes, batch, feats), kind),
            pltpu.VMEM((4, batch, feats), kind),
            dma((2, 3)),
            dma((2, replicas * 4 * subs)),
            dma((2, replicas * 4)),
            dma((2,)),
            dma((8,)),
            dma((planes,)),
            dma((planes,)),
            dma((2, planes)),
            dma((2, planes)),
            dma((3,)),
            dma((3,)),
        ],
        compiler_params=pltpu.CompilerParams(
            collective_id=0, has_side_effects=True, vmem_limit_bytes=8 * 2**20
        ),
        cost_estimate=pl.CostEstimate(
            flops=2 * 10**11, bytes_accessed=2 * width * query_cols, transcendentals=0
        ),
        name="weight_exchange",
    )(
        *(
            pltpu.with_memory_space_constraint(operand, pltpu.HBM)
            for operand in (
                token_ids.reshape(1, tokens),
                norm_gain.reshape(-1, lanes),
                lengths,
                embed_table,
                w_query,
                w_keyvalue,
                key_cache,
                value_cache,
            )
        )
    )


def finish_kernel(
    query_acc,
    spread_ref,
    query_all,
    pair_all,
    key_ref,
    value_ref,
    length_ref,
    query_ref,
    pair_ref,
    context_ref,
    query_heads,
    scores_ref,
    weights_ref,
    context_heads,
    context_hold,
    sems,
    context_sem,
):
    pair_cols = pair_all.shape[1]
    batch, group, head_size = query_heads.shape
    parts = sems.shape[1]
    stores = []
    for c, (held, out) in enumerate(((query_all, query_ref), (pair_all, pair_ref))):
        size = held.shape[0] // parts
        for i in range(parts):
            where = pl.ds(i * size, size)
            stores.append(pltpu.make_async_copy(held.at[where], out.at[where], sems.at[c, i]))
    for copy in stores:
        copy.start()

    query = query_acc[...].astype(jnp.bfloat16).astype(jnp.float32)
    for j in range(group):
        query_heads[:, j, :] = query[:, j * head_size : (j + 1) * head_size]
    for s in range(batch):
        scores_ref[s] = lax.dot_general(
            query_heads[s].astype(jnp.bfloat16),
            key_ref[s],
            (((1,), (1,)), ((), ())),
            preferred_element_type=jnp.float32,
        )

    block = 2048

    def project(i, pair):
        here = pl.ds(pl.multiple_of(i * block, block), block)
        return pair + jnp.dot(
            spread_ref[:, here], pair_all[here, :], preferred_element_type=jnp.float32
        )

    pair = lax.fori_loop(
        0,
        pair_all.shape[0] // block,
        project,
        jnp.zeros((2 * batch, pair_cols), jnp.float32),
    )
    pair = pair.astype(jnp.bfloat16).astype(jnp.float32)

    scale = head_size ** (-0.5)
    slots = key_ref.shape[1]
    position = lax.broadcasted_iota(jnp.int32, (group, slots), 1)
    own_weights = []
    for s in range(batch):
        scores = jnp.where(position < length_ref[s, :, 0:1], scores_ref[s] * scale, -jnp.inf)
        own = jnp.sum(query_heads[s] * pair[s : s + 1], axis=1, keepdims=True) * scale
        top = jnp.maximum(jnp.max(scores, axis=1, keepdims=True), own)
        weights = jnp.exp(scores - top)
        own_weight = jnp.exp(own - top)
        share = 1.0 / (jnp.sum(weights, axis=1, keepdims=True) + own_weight)
        weights_ref[s] = (weights * share).astype(jnp.bfloat16)
        own_weights.append((own_weight * share).astype(jnp.bfloat16).astype(jnp.float32))
    for s in range(batch):
        context_heads[s] = (
            jnp.dot(weights_ref[s], value_ref[s], preferred_element_type=jnp.float32)
            + own_weights[s] * pair[batch + s : batch + s + 1]
        )
    for j in range(group):
        context_hold[:, j * head_size : (j + 1) * head_size] = context_heads[:, j, :].astype(
            context_hold.dtype
        )
    context = pltpu.make_async_copy(context_hold, context_ref, context_sem)
    context.start()
    for copy in stores:
        copy.wait()
    context.wait()


def finish(query_acc, spread, query_all, pair_all, keys, values, lengths):
    batch, query_cols = query_acc.shape
    width, _, pair_cols = pair_all.shape
    kind = query_all.dtype
    slots, head_size = keys.shape[1], keys.shape[2]
    group = query_cols // head_size
    pair_flat = pair_all.reshape(2 * width, pair_cols)
    vmem = pl.BlockSpec(memory_space=pltpu.VMEM)
    shape = jax.ShapeDtypeStruct
    query_out, pair_out, context = pl.pallas_call(
        finish_kernel,
        out_shape=(
            shape(query_all.shape, kind),
            shape(pair_flat.shape, kind),
            shape((batch, query_cols), kind),
        ),
        in_specs=[vmem] * 7,
        out_specs=(pl.BlockSpec(memory_space=pltpu.HBM),) * 3,
        scratch_shapes=[
            pltpu.VMEM((batch, group, head_size), jnp.float32),
            pltpu.VMEM((batch, group, slots), jnp.float32),
            pltpu.VMEM((batch, group, slots), kind),
            pltpu.VMEM((batch, group, head_size), jnp.float32),
            pltpu.VMEM((batch, query_cols), kind),
            pltpu.SemaphoreType.DMA((2, 4)),
            pltpu.SemaphoreType.DMA(()),
        ],
        compiler_params=pltpu.CompilerParams(vmem_limit_bytes=8 * 2**20),
        cost_estimate=pl.CostEstimate(
            flops=8 * batch * width * pair_cols,
            bytes_accessed=4 * width * (query_cols + 2 * pair_cols),
            transcendentals=0,
        ),
        name="attend_and_store",
    )(query_acc, spread, query_all, pair_flat, keys, values, lengths)
    return context, query_out, pair_out.reshape(width, 2, pair_cols)


def per_device_line(
    planes,
    token_ids,
    embed_table,
    norm_gain,
    w_query,
    w_keyvalue,
    key_cache,
    value_cache,
    cache_lengths,
):
    query_all, pair_all, keys, values, lengths, _, spread, query_acc = exchange(
        token_ids,
        norm_gain,
        embed_table,
        w_query,
        w_keyvalue,
        key_cache,
        value_cache,
        cache_lengths,
        planes,
    )
    return finish(query_acc, spread, query_all, pair_all, keys, values, lengths)


def solution(mesh):
    replicas, tp = mesh.shape["replica"], mesh.shape["tp"]

    def body(*args):
        key_cache, lengths, w_keyvalue = args[5], args[7], args[4]
        one_head = w_keyvalue.shape[2] == tp * key_cache.shape[2]
        own_rows = key_cache.shape[0] == lengths.shape[0]
        if tp == 4 and replicas % 2 == 0 and replicas > 6 and one_head and own_rows:
            return per_device_line(replicas // 2, *args)
        return per_device(*args)

    return jax.shard_map(
        body,
        mesh=mesh,
        in_specs=(
            P(),
            P("replica", "tp"),
            P(),
            P(("replica", "tp"), None),
            P(("replica", "tp"), None, None),
            P(("replica", "tp"), None, None),
            P(("replica", "tp"), None, None),
            P("replica"),
        ),
        out_specs=(P(("replica", "tp"), None), P(None, "tp"), P(None, None, "tp")),
        check_vma=False,
    )
```

```python
import functools

import jax
import jax.numpy as jnp
from jax import lax
from jax.experimental import pallas as pl
from jax.experimental.pallas import tpu as pltpu
from jax.sharding import PartitionSpec as P


def attend(query, keys, values, key_new, value_new, lengths):
    scale = query.shape[-1] ** (-0.5)
    scores = jnp.einsum("rgd,rcd->rgc", query, keys, preferred_element_type=jnp.float32) * scale
    position = lax.broadcasted_iota(jnp.int32, scores.shape, 2)
    scores = jnp.where(position < lengths[:, None, None], scores, -jnp.inf)
    own = jnp.einsum("rgd,rd->rg", query, key_new, preferred_element_type=jnp.float32) * scale
    top = jnp.maximum(jnp.max(scores, axis=2), own)
    weights = jnp.exp(scores - top[:, :, None])
    own_weight = jnp.exp(own - top)
    total = jnp.sum(weights, axis=2) + own_weight
    weights = (weights / total[:, :, None]).astype(jnp.bfloat16)
    own_weight = (own_weight / total).astype(jnp.bfloat16)
    context = jnp.einsum("rgc,rcd->rgd", weights, values, preferred_element_type=jnp.float32)
    context = (
        context
        + own_weight.astype(jnp.float32)[:, :, None] * value_new.astype(jnp.float32)[:, None, :]
    )
    return context.astype(jnp.bfloat16)


def per_device(
    token_ids, embed_table, norm_gain, w_query, w_keyvalue, key_cache, value_cache, cache_lengths
):
    group_index = lax.axis_index("replica")
    tp_index = lax.axis_index("tp")
    vocab_rows, feature_cols = embed_table.shape
    batch = cache_lengths.shape[0]
    first_id = group_index * vocab_rows
    picked = token_ids - first_id
    columns = lax.broadcasted_iota(jnp.int32, (batch * lax.axis_size("replica"), vocab_rows), 1)
    onehot = (picked[:, None] == columns).astype(jnp.bfloat16)
    embedded = lax.psum_scatter(
        jnp.dot(onehot, embed_table, preferred_element_type=jnp.float32),
        "replica",
        scatter_dimension=0,
        tiled=True,
    ).astype(jnp.bfloat16)
    whole = lax.all_gather(embedded, "tp", axis=1, tiled=True)
    values32 = whole.astype(jnp.float32)
    mean_square = jnp.mean(values32 * values32, axis=1, keepdims=True)
    normed = (values32 * lax.rsqrt(mean_square + 1e-05) * norm_gain.astype(jnp.float32)).astype(
        jnp.bfloat16
    )
    width = normed.shape[1]
    query_rows = w_query.reshape(w_query.shape[0], 1, w_query.shape[1])
    query_mid, pair_mid = (
        lax.all_to_all(query_rows, "tp", split_axis=2, concat_axis=0, tiled=True),
        lax.all_to_all(w_keyvalue, "tp", split_axis=2, concat_axis=0, tiled=True),
    )
    flat_query = query_mid.reshape(query_mid.shape[0], query_mid.shape[2])
    pair_cols = pair_mid.shape[2]
    flat_pair = pair_mid.reshape(pair_mid.shape[0], 2 * pair_cols)
    query_full, pair_full = (
        lax.all_gather(flat_query, "replica", axis=0, tiled=True),
        lax.all_gather(flat_pair, "replica", axis=0, tiled=True),
    )
    query_acc = jnp.dot(normed, query_full, preferred_element_type=jnp.float32)
    pair_acc = jnp.dot(normed, pair_full, preferred_element_type=jnp.float32)
    query_local = query_acc.astype(jnp.bfloat16)
    pair_local = pair_acc.astype(jnp.bfloat16).reshape(batch, 2, pair_cols)
    query_heads, pair_heads = (
        lax.all_gather(query_local, "tp", axis=1, tiled=True),
        lax.all_gather(pair_local, "tp", axis=2, tiled=True),
    )
    head_size = key_cache.shape[2]
    kv_heads = pair_heads.shape[2] // head_size
    group = query_heads.shape[1] // (kv_heads * head_size)
    rows_here = key_cache.shape[0]
    first_row = tp_index * rows_here
    query_grouped = (
        query_heads.reshape(batch, kv_heads, group, head_size)
        .transpose(1, 0, 2, 3)
        .reshape(kv_heads * batch, group, head_size)
    )
    key_grouped = (
        pair_heads[:, 0]
        .reshape(batch, kv_heads, head_size)
        .transpose(1, 0, 2)
        .reshape(kv_heads * batch, head_size)
    )
    value_grouped = (
        pair_heads[:, 1]
        .reshape(batch, kv_heads, head_size)
        .transpose(1, 0, 2)
        .reshape(kv_heads * batch, head_size)
    )
    query_mine = lax.dynamic_slice_in_dim(query_grouped, first_row, rows_here, 0)
    key_mine = lax.dynamic_slice_in_dim(key_grouped, first_row, rows_here, 0)
    value_mine = lax.dynamic_slice_in_dim(value_grouped, first_row, rows_here, 0)
    sequence = (first_row + lax.broadcasted_iota(jnp.int32, (rows_here,), 0)) % batch
    matches = sequence[:, None] == lax.broadcasted_iota(jnp.int32, (rows_here, batch), 1)
    row_lengths = jnp.sum(jnp.where(matches, cache_lengths[None, :], 0), axis=1)
    context = attend(query_mine, key_cache, value_cache, key_mine, value_mine, row_lengths)
    context = context.reshape(rows_here, group * head_size)
    return (context, query_full, pair_full.reshape(width, 2, pair_cols))


MESH = pl.DeviceIdType.MESH


def exchange_kernel(
    planes,
    cuts,
    token_in,
    gain_in,
    length_in,
    table_in,
    query_in,
    pair_in,
    key_in,
    value_in,
    query_out,
    pair_out,
    key_out,
    value_out,
    length_out,
    normed_ref,
    spread_ref,
    query_acc,
    token_hold,
    gain_hold,
    gain_wide,
    length_hold,
    table_hold,
    onehot_ref,
    part_ref,
    given,
    joined,
    sums,
    brought,
    pieces,
    send_sem,
    recv_sem,
    hand_recv,
    across_sem,
    local_sem,
    give_send,
    give_recv,
    sum_send,
    sum_recv,
    piece_send,
    piece_recv,
    corner_sem,
):
    r, t = lax.axis_index("replica"), lax.axis_index("tp")
    replicas = 2 * planes
    z, k = r // 2, lax.rem(r, 2)
    ty, tx = t // 2, lax.rem(t, 2)
    rows, query_cols = query_in.shape[0], query_out.shape[1]
    pair_cols = pair_out.shape[2]
    finest = max(cuts.values())
    batch, feats = pieces.shape[1], pieces.shape[2]
    other = [t, ty * 2 + 1 - tx, (1 - ty) * 2 + tx, 3 - t]
    partner = z * 2 + 1 - k

    def piece_id(plane, core, tp):
        return (plane * 2 + core) * 4 + tp

    def part_of(ref, pid, s, cut):
        sub = rows // cut
        return ref.at[pl.ds(pl.multiple_of(pid * rows + s * sub, sub), sub)]

    mine = piece_id(z, k, t)

    def columns(tp, first, count):
        return (
            query_in.at[
                pl.ds(first, count), pl.ds(pl.multiple_of(tp * query_cols, query_cols), query_cols)
            ],
            pair_in.at[
                pl.ds(first, count), :, pl.ds(pl.multiple_of(tp * pair_cols, pair_cols), pair_cols)
            ],
        )

    own = columns(t, 0, rows)
    where_own = pl.ds(pl.multiple_of(mine * rows, rows), rows)
    bring = [
        pltpu.make_async_copy(own[0], query_out.at[where_own], local_sem.at[0]),
        pltpu.make_async_copy(own[1], pair_out.at[where_own], local_sem.at[1]),
    ]
    fetch = [
        pltpu.make_async_copy(token_in, token_hold, local_sem.at[2]),
        pltpu.make_async_copy(table_in, table_hold, local_sem.at[3]),
        pltpu.make_async_copy(gain_in, gain_hold, local_sem.at[4]),
        pltpu.make_async_copy(length_in, length_hold, local_sem.at[5]),
        pltpu.make_async_copy(key_in, key_out, local_sem.at[6]),
        pltpu.make_async_copy(value_in, value_out, local_sem.at[7]),
    ]
    for copy in bring:
        copy.start()

    barrier = pltpu.get_barrier_semaphore()
    for j in range(1, 3):
        pl.semaphore_signal(barrier, inc=1, device_id=(r, other[j]), device_id_type=MESH)
    pl.semaphore_signal(barrier, inc=1, device_id=(partner, t), device_id_type=MESH)
    above, below = lax.rem(r + 2, replicas), lax.rem(r + replicas - 2, replicas)

    @pl.when(z < planes - 1)
    def _():
        pl.semaphore_signal(barrier, inc=1, device_id=(above, t), device_id_type=MESH)

    @pl.when(z > 0)
    def _():
        pl.semaphore_signal(barrier, inc=1, device_id=(below, t), device_id_type=MESH)

    for copy in fetch[:2]:
        copy.start()
    pl.semaphore_wait(barrier, 3 + jnp.minimum(z, 1) + jnp.minimum(planes - 1 - z, 1))

    held = (query_out, pair_out)

    def landed(c, pid, s, cut):
        place = part_of(held[c], pid, s, cut)
        pltpu.make_async_copy(place, place, recv_sem.at[c, pid * finest + s]).wait()

    def send(c, pid, s, cut, way, target):
        place = part_of(held[c], pid, s, cut)
        pltpu.make_async_remote_copy(
            src_ref=place,
            dst_ref=place,
            send_sem=send_sem.at[c, way],
            recv_sem=hand_recv.at[c, pid] if way == 2 else recv_sem.at[c, pid * finest + s],
            device_id=target,
            device_id_type=MESH,
        ).start()

    def sent(way, pieces_sent):
        for c, out in enumerate(held):
            place = out.at[0 : pieces_sent * rows]
            pltpu.make_async_copy(place, place, send_sem.at[c, way]).wait()

    def handed(pid):
        for c, out in enumerate(held):
            place = out.at[pl.ds(pl.multiple_of(pid * rows, rows), rows)]
            pltpu.make_async_copy(place, place, hand_recv.at[c, pid]).wait()

    def across(j):
        cut = cuts["across", j]
        sub = rows // cut

        def act(s, carry):
            sources = columns(other[j], pl.multiple_of(s * sub, sub), sub)
            for c, source in enumerate(sources):
                pltpu.make_async_remote_copy(
                    src_ref=source,
                    dst_ref=part_of(held[c], mine, s, cut),
                    send_sem=across_sem.at[c],
                    recv_sem=recv_sem.at[c, mine * finest + s],
                    device_id=(r, other[j]),
                    device_id_type=MESH,
                ).start()
            return carry

        lax.fori_loop(0, cut, act, 0)

    def forward(pid, came_in, go_out, up, down):
        groups = min(came_in, go_out) if came_in else go_out

        def act(g, carry):
            for c in range(2):
                for i in range(came_in // groups):
                    landed(c, pid, g * (came_in // groups) + i, came_in)
                for i in range(go_out // groups):
                    s = g * (go_out // groups) + i
                    if up:

                        @pl.when(z < planes - 1)
                        def _():
                            send(c, pid, s, go_out, 0, (above, t))

                    if down:

                        @pl.when(z > 0)
                        def _():
                            send(c, pid, s, go_out, 1, (below, t))

                send(c, pid, g, groups, 2, (partner, t))
            return carry

        lax.fori_loop(0, groups, act, 0)

    def out_cut(far, j):
        return cuts.get((far, j), 1)

    def near(j):
        came_in = cuts["across", j] if j else 0
        forward(piece_id(z, k, other[j]), came_in, out_cut(0, j), True, True)

    def planes_at(far, act):
        if far == 0:
            act(z, True)
            return

        @pl.when(z >= far)
        def _():
            act(lax.rem(z + planes - far, planes), True)

        @pl.when(z + far < planes)
        def _():
            act(lax.rem(z + far, planes), False)

    def far_away(far, j):
        def act(plane, up):
            pid = piece_id(plane, k, other[j])
            forward(pid, out_cut(far - 1, j), out_cut(far, j), up, not up)

        planes_at(far, act)

    def multiply(far, j):
        def both(plane, up):
            def add(turn, carry):
                pid = piece_id(plane, jnp.where(turn == 0, k, 1 - k), other[j])

                @pl.when(turn == 1)
                def _():
                    handed(pid)

                where = pl.ds(pl.multiple_of(pid * rows, rows), rows)
                query_acc[...] += jnp.dot(
                    normed_ref[:, where], query_out[where, :], preferred_element_type=jnp.float32
                )
                return carry

            lax.fori_loop(0, 2, add, 0)

        planes_at(far, both)

    for copy in bring:
        copy.wait()

    near(0)
    pl.semaphore_signal(corner_sem, inc=1, device_id=(r, other[1]), device_id_type=MESH)
    across(1)
    across(2)
    for copy in fetch[2:]:
        copy.start()
    pl.semaphore_wait(corner_sem, 1)
    across(3)

    gives = [
        pltpu.make_async_remote_copy(
            src_ref=part_ref.at[plane, 1 - k],
            dst_ref=given.at[plane],
            send_sem=give_send.at[plane],
            recv_sem=give_recv.at[plane],
            device_id=(partner, t),
            device_id_type=MESH,
        )
        for plane in range(planes)
    ]

    last = planes - 1

    def passing(hop, wait=False):
        for way in range(2):
            for plane in range(planes - 1):
                if plane != hop and not wait:
                    continue
                place = plane if way == 0 else last - plane
                target = (place + 1 if way == 0 else place - 1) * 2 + k
                dests = range(place + 1, planes) if way == 0 else range(place)

                @pl.when(z == place)
                def _():
                    for dest in dests:
                        if plane > 0 and not wait:
                            came(way, dest)
                            total = joined[dest].astype(jnp.float32) + brought[
                                way, dest
                            ].astype(jnp.float32)
                            sums[way, dest] = total.astype(jnp.bfloat16)
                        copy = pltpu.make_async_remote_copy(
                            src_ref=sums.at[way, dest] if plane > 0 else joined.at[dest],
                            dst_ref=brought.at[way, dest],
                            send_sem=sum_send.at[way, dest],
                            recv_sem=sum_recv.at[way, dest],
                            device_id=(target, t),
                            device_id_type=MESH,
                        )
                        copy.wait_send() if wait else copy.start()

    def came(way, dest):
        place = brought.at[way, dest]
        pltpu.make_async_copy(place, place, sum_recv.at[way, dest]).wait()

    gather = [
        pltpu.make_async_remote_copy(
            src_ref=pieces.at[t],
            dst_ref=pieces.at[t],
            send_sem=piece_send.at[j - 1],
            recv_sem=piece_recv.at[j - 1],
            device_id=(r, other[j]),
            device_id_type=MESH,
        )
        for j in range(1, 4)
    ]

    def select_rows():
        fetch[0].wait()
        vocab_rows = table_hold.shape[0]
        tokens = token_hold.shape[1]
        lanes = 128
        wanted = jnp.broadcast_to(token_hold[...] - r * vocab_rows, (lanes, tokens)).T
        lane = lax.broadcasted_iota(jnp.int32, (tokens, lanes), 1)
        for first in range(0, vocab_rows, lanes):
            onehot_ref[:, first : first + lanes] = (wanted == lane + first).astype(
                onehot_ref.dtype
            )
        fetch[1].wait()
        block = 256

        def select(i, carry):
            where = pl.ds(pl.multiple_of(i * block, block), block)
            rows_here = jnp.dot(
                onehot_ref[...], table_hold[:, where], preferred_element_type=jnp.float32
            ).astype(jnp.bfloat16)
            part_ref[:, :, :, where] = rows_here.reshape(planes, 2, batch, block)
            return carry

        lax.fori_loop(0, feats // block, select, 0)

    def join():
        for copy in gives:
            copy.wait()
        for plane in range(planes):
            kept = part_ref[plane, k].astype(jnp.float32)
            joined[plane] = (kept + given[plane].astype(jnp.float32)).astype(jnp.bfloat16)

    def sum_all():
        for dest in range(planes):

            @pl.when(z == dest)
            def _():
                total = joined[dest].astype(jnp.float32)
                for way in range(2):
                    if dest != (0 if way == 0 else last):
                        came(way, dest)
                        total = total + brought[way, dest].astype(jnp.float32)
                pieces[t] = total.astype(jnp.bfloat16)

    def normalise():
        fetch[2].wait()
        gain_wide[...] = gain_hold[...].astype(jnp.float32)
        for copy in gather:
            copy.wait()
        square = jnp.zeros((batch, 1), jnp.float32)
        for i in range(4):
            part = pieces[i].astype(jnp.float32)
            square = square + jnp.sum(part * part, axis=1, keepdims=True)
        factor = lax.rsqrt(square / (4 * feats) + 1e-05)
        lanes = gain_wide.shape[1]
        blocks = feats // lanes
        for i in range(4):

            def scaled(b, carry):
                part = pieces[i, :, pl.ds(pl.multiple_of(b * lanes, lanes), lanes)]
                gain = gain_wide[pl.ds(i * blocks + b, 1), :]
                where = pl.ds(pl.multiple_of(i * feats + b * lanes, lanes), lanes)
                normed_ref[:, where] = (part.astype(jnp.float32) * factor * gain).astype(
                    jnp.bfloat16
                )
                return carry

            lax.fori_loop(0, blocks, scaled, 0)
        block = 256
        line = lax.broadcasted_iota(jnp.int32, (block, 2 * block), 0)
        column = lax.broadcasted_iota(jnp.int32, (block, 2 * block), 1)
        even = (column == 2 * line).astype(jnp.bfloat16)
        odd = (column == 2 * line + 1).astype(jnp.bfloat16)

        def spread(i, carry):
            part = normed_ref[:, pl.ds(pl.multiple_of(i * block, block), block)]
            where = pl.ds(pl.multiple_of(i * 2 * block, 2 * block), 2 * block)
            spread_ref[0:batch, where] = jnp.dot(
                part, even, preferred_element_type=jnp.float32
            ).astype(jnp.bfloat16)
            spread_ref[batch : 2 * batch, where] = jnp.dot(
                part, odd, preferred_element_type=jnp.float32
            ).astype(jnp.bfloat16)
            return carry

        lax.fori_loop(0, 4 * feats // block, spread, 0)

    def lengths():
        fetch[3].wait()
        group = length_out.shape[1]
        for s in range(batch):
            length_out[s] = jnp.full((group, length_out.shape[2]), length_hold[s], jnp.int32)

    select_rows()
    for copy in gives:
        copy.start()
    join()
    passing(0)
    order = [(0, 1), (0, 2), (1, 0), (0, 3)]
    order += [(far, j) for far in range(1, planes) for j in range(4) if (far, j) != (1, 0)]
    middle = len(order) - 5
    for step, (far, j) in enumerate(order):
        near(j) if far == 0 else far_away(far, j)
        if step == 1:
            passing(1)
        if step > 4 and step - 3 < planes - 1:
            passing(step - 3)
        if step == middle - 1:
            sum_all()
            for copy in gather:
                copy.start()
        if step == middle:
            normalise()
            lengths()
            query_acc[...] = jnp.zeros_like(query_acc)
            for past in [(0, 0)] + order[:middle]:
                multiply(*past)
        if step > middle:
            multiply(*order[step - 1])

    for copy in fetch[4:]:
        copy.wait()
    for c, out in enumerate((query_out, pair_out)):
        place = out.at[0 : 3 * rows]
        pltpu.make_async_copy(place, place, across_sem.at[c]).wait()
    passing(0, wait=True)
    multiply(*order[-1])
    for place in range(planes):

        @pl.when(z == place)
        def _():
            if place < last:
                sent(0, 4 * (place + 1))
            if place > 0:
                sent(1, 4 * (planes - place))

    sent(2, 4 * planes)


def exchange(
    token_ids, norm_gain, embed_table, w_query, w_keyvalue, key_cache, value_cache, lengths, planes
):
    rows, all_query = w_query.shape
    query_cols, pair_cols = all_query // 4, w_keyvalue.shape[2] // 4
    replicas = 2 * planes
    width = rows * replicas * 4
    feats = embed_table.shape[1]
    kind = w_query.dtype
    batch, head_size = lengths.shape[0], key_cache.shape[2]
    group = query_cols // head_size
    tokens = token_ids.shape[0]
    lanes = 128
    cuts = {("across", 1): 1, ("across", 2): 1, ("across", 3): 1}
    cuts |= {(0, 0): 1, (0, 1): 1, (0, 2): 1, (0, 3): 1}
    anywhere = pl.BlockSpec(memory_space=pl.ANY)
    vmem = pl.BlockSpec(memory_space=pltpu.VMEM)
    dma = pltpu.SemaphoreType.DMA
    shape = jax.ShapeDtypeStruct
    return pl.pallas_call(
        functools.partial(exchange_kernel, planes, cuts),
        out_shape=(
            pltpu.VMEM((width, query_cols), kind),
            pltpu.VMEM((width, 2, pair_cols), kind),
            pltpu.VMEM(key_cache.shape, kind),
            pltpu.VMEM(value_cache.shape, kind),
            pltpu.VMEM((batch, group, head_size), jnp.int32),
            pltpu.VMEM((batch, width), kind),
            pltpu.VMEM((2 * batch, 2 * width), kind),
            pltpu.VMEM((batch, query_cols), jnp.float32),
        ),
        in_specs=[anywhere] * 8,
        out_specs=(vmem,) * 8,
        scratch_shapes=[
            pltpu.VMEM((1, tokens), jnp.int32),
            pltpu.VMEM((width // lanes, lanes), kind),
            pltpu.VMEM((width // lanes, lanes), jnp.float32),
            pltpu.SMEM((batch,), jnp.int32),
            pltpu.VMEM(embed_table.shape, kind),
            pltpu.VMEM((tokens, embed_table.shape[0]), kind),
            pltpu.VMEM((planes, 2, batch, feats), kind),
            pltpu.VMEM((planes, batch, feats), kind),
            pltpu.VMEM((planes, batch, feats), kind),
            pltpu.VMEM((2, planes, batch, feats), kind),
            pltpu.VMEM((2, planes, batch, feats), kind),
            pltpu.VMEM((4, batch, feats), kind),
            dma((2, 3)),
            dma((2, replicas * 4 * max(cuts.values()))),
            dma((2, replicas * 4)),
            dma((2,)),
            dma((8,)),
            dma((planes,)),
            dma((planes,)),
            dma((2, planes)),
            dma((2, planes)),
            dma((3,)),
            dma((3,)),
            pltpu.SemaphoreType.REGULAR,
        ],
        compiler_params=pltpu.CompilerParams(
            collective_id=0, has_side_effects=True, vmem_limit_bytes=8 * 2**20
        ),
        cost_estimate=pl.CostEstimate(
            flops=2 * 10**11, bytes_accessed=2 * width * query_cols, transcendentals=0
        ),
        name="weight_exchange",
    )(
        *(
            pltpu.with_memory_space_constraint(operand, pltpu.HBM)
            for operand in (
                token_ids.reshape(1, tokens),
                norm_gain.reshape(-1, lanes),
                lengths,
                embed_table,
                w_query,
                w_keyvalue,
                key_cache,
                value_cache,
            )
        )
    )


def finish_kernel(
    query_acc,
    spread_ref,
    query_all,
    pair_all,
    key_ref,
    value_ref,
    length_ref,
    query_ref,
    pair_ref,
    context_ref,
    query_heads,
    scores_ref,
    weights_ref,
    context_heads,
    context_hold,
    sems,
    context_sem,
):
    pair_cols = pair_all.shape[1]
    batch, group, head_size = query_heads.shape
    parts = sems.shape[1]
    stores = []
    for c, (held, out) in enumerate(((query_all, query_ref), (pair_all, pair_ref))):
        size = held.shape[0] // parts
        for i in range(parts):
            where = pl.ds(i * size, size)
            stores.append(pltpu.make_async_copy(held.at[where], out.at[where], sems.at[c, i]))
    for copy in stores:
        copy.start()

    query = query_acc[...].astype(jnp.bfloat16).astype(jnp.float32)
    for j in range(group):
        query_heads[:, j, :] = query[:, j * head_size : (j + 1) * head_size]
    for s in range(batch):
        scores_ref[s] = lax.dot_general(
            query_heads[s].astype(jnp.bfloat16),
            key_ref[s],
            (((1,), (1,)), ((), ())),
            preferred_element_type=jnp.float32,
        )

    block = 2048

    def project(i, pair):
        here = pl.ds(pl.multiple_of(i * block, block), block)
        return pair + jnp.dot(
            spread_ref[:, here], pair_all[here, :], preferred_element_type=jnp.float32
        )

    pair = lax.fori_loop(
        0,
        pair_all.shape[0] // block,
        project,
        jnp.zeros((2 * batch, pair_cols), jnp.float32),
    )
    pair = pair.astype(jnp.bfloat16).astype(jnp.float32)

    scale = head_size ** (-0.5)
    slots = key_ref.shape[1]
    position = lax.broadcasted_iota(jnp.int32, (group, slots), 1)
    own_weights = []
    for s in range(batch):
        scores = jnp.where(position < length_ref[s, :, 0:1], scores_ref[s] * scale, -jnp.inf)
        own = jnp.sum(query_heads[s] * pair[s : s + 1], axis=1, keepdims=True) * scale
        top = jnp.maximum(jnp.max(scores, axis=1, keepdims=True), own)
        weights = jnp.exp(scores - top)
        own_weight = jnp.exp(own - top)
        share = 1.0 / (jnp.sum(weights, axis=1, keepdims=True) + own_weight)
        weights_ref[s] = (weights * share).astype(jnp.bfloat16)
        own_weights.append((own_weight * share).astype(jnp.bfloat16).astype(jnp.float32))
    for s in range(batch):
        context_heads[s] = (
            jnp.dot(weights_ref[s], value_ref[s], preferred_element_type=jnp.float32)
            + own_weights[s] * pair[batch + s : batch + s + 1]
        )
    for j in range(group):
        context_hold[:, j * head_size : (j + 1) * head_size] = context_heads[:, j, :].astype(
            context_hold.dtype
        )
    context = pltpu.make_async_copy(context_hold, context_ref, context_sem)
    context.start()
    for copy in stores:
        copy.wait()
    context.wait()


def finish(query_acc, spread, query_all, pair_all, keys, values, lengths):
    batch, query_cols = query_acc.shape
    width, _, pair_cols = pair_all.shape
    kind = query_all.dtype
    slots, head_size = keys.shape[1], keys.shape[2]
    group = query_cols // head_size
    pair_flat = pair_all.reshape(2 * width, pair_cols)
    vmem = pl.BlockSpec(memory_space=pltpu.VMEM)
    shape = jax.ShapeDtypeStruct
    query_out, pair_out, context = pl.pallas_call(
        finish_kernel,
        out_shape=(
            shape(query_all.shape, kind),
            shape(pair_flat.shape, kind),
            shape((batch, query_cols), kind),
        ),
        in_specs=[vmem] * 7,
        out_specs=(pl.BlockSpec(memory_space=pltpu.HBM),) * 3,
        scratch_shapes=[
            pltpu.VMEM((batch, group, head_size), jnp.float32),
            pltpu.VMEM((batch, group, slots), jnp.float32),
            pltpu.VMEM((batch, group, slots), kind),
            pltpu.VMEM((batch, group, head_size), jnp.float32),
            pltpu.VMEM((batch, query_cols), kind),
            pltpu.SemaphoreType.DMA((2, 4)),
            pltpu.SemaphoreType.DMA(()),
        ],
        compiler_params=pltpu.CompilerParams(vmem_limit_bytes=8 * 2**20),
        cost_estimate=pl.CostEstimate(
            flops=8 * batch * width * pair_cols,
            bytes_accessed=4 * width * (query_cols + 2 * pair_cols),
            transcendentals=0,
        ),
        name="attend_and_store",
    )(query_acc, spread, query_all, pair_flat, keys, values, lengths)
    return context, query_out, pair_out.reshape(width, 2, pair_cols)


def per_device_line(
    planes,
    token_ids,
    embed_table,
    norm_gain,
    w_query,
    w_keyvalue,
    key_cache,
    value_cache,
    cache_lengths,
):
    query_all, pair_all, keys, values, lengths, _, spread, query_acc = exchange(
        token_ids,
        norm_gain,
        embed_table,
        w_query,
        w_keyvalue,
        key_cache,
        value_cache,
        cache_lengths,
        planes,
    )
    return finish(query_acc, spread, query_all, pair_all, keys, values, lengths)


def solution(mesh):
    replicas, tp = mesh.shape["replica"], mesh.shape["tp"]

    def body(*args):
        key_cache, lengths, w_keyvalue = args[5], args[7], args[4]
        one_head = w_keyvalue.shape[2] == tp * key_cache.shape[2]
        own_rows = key_cache.shape[0] == lengths.shape[0]
        if tp == 4 and replicas % 2 == 0 and replicas > 6 and one_head and own_rows:
            return per_device_line(replicas // 2, *args)
        return per_device(*args)

    return jax.shard_map(
        body,
        mesh=mesh,
        in_specs=(
            P(),
            P("replica", "tp"),
            P(),
            P(("replica", "tp"), None),
            P(("replica", "tp"), None, None),
            P(("replica", "tp"), None, None),
            P(("replica", "tp"), None, None),
            P("replica"),
        ),
        out_specs=(P(("replica", "tp"), None), P(None, "tp"), P(None, None, "tp")),
        check_vma=False,
    )
```

```python
import functools

import jax
import jax.numpy as jnp
from jax import lax
from jax.experimental import pallas as pl
from jax.experimental.pallas import tpu as pltpu
from jax.sharding import PartitionSpec as P


def attend(query, keys, values, key_new, value_new, lengths):
    scale = query.shape[-1] ** (-0.5)
    scores = jnp.einsum("rgd,rcd->rgc", query, keys, preferred_element_type=jnp.float32) * scale
    position = lax.broadcasted_iota(jnp.int32, scores.shape, 2)
    scores = jnp.where(position < lengths[:, None, None], scores, -jnp.inf)
    own = jnp.einsum("rgd,rd->rg", query, key_new, preferred_element_type=jnp.float32) * scale
    top = jnp.maximum(jnp.max(scores, axis=2), own)
    weights = jnp.exp(scores - top[:, :, None])
    own_weight = jnp.exp(own - top)
    total = jnp.sum(weights, axis=2) + own_weight
    weights = (weights / total[:, :, None]).astype(jnp.bfloat16)
    own_weight = (own_weight / total).astype(jnp.bfloat16)
    context = jnp.einsum("rgc,rcd->rgd", weights, values, preferred_element_type=jnp.float32)
    context = (
        context
        + own_weight.astype(jnp.float32)[:, :, None] * value_new.astype(jnp.float32)[:, None, :]
    )
    return context.astype(jnp.bfloat16)


def per_device(
    token_ids, embed_table, norm_gain, w_query, w_keyvalue, key_cache, value_cache, cache_lengths
):
    group_index = lax.axis_index("replica")
    tp_index = lax.axis_index("tp")
    vocab_rows, feature_cols = embed_table.shape
    batch = cache_lengths.shape[0]
    first_id = group_index * vocab_rows
    picked = token_ids - first_id
    columns = lax.broadcasted_iota(jnp.int32, (batch * lax.axis_size("replica"), vocab_rows), 1)
    onehot = (picked[:, None] == columns).astype(jnp.bfloat16)
    embedded = lax.psum_scatter(
        jnp.dot(onehot, embed_table, preferred_element_type=jnp.float32),
        "replica",
        scatter_dimension=0,
        tiled=True,
    ).astype(jnp.bfloat16)
    whole = lax.all_gather(embedded, "tp", axis=1, tiled=True)
    values32 = whole.astype(jnp.float32)
    mean_square = jnp.mean(values32 * values32, axis=1, keepdims=True)
    normed = (values32 * lax.rsqrt(mean_square + 1e-05) * norm_gain.astype(jnp.float32)).astype(
        jnp.bfloat16
    )
    width = normed.shape[1]
    query_rows = w_query.reshape(w_query.shape[0], 1, w_query.shape[1])
    query_mid, pair_mid = (
        lax.all_to_all(query_rows, "tp", split_axis=2, concat_axis=0, tiled=True),
        lax.all_to_all(w_keyvalue, "tp", split_axis=2, concat_axis=0, tiled=True),
    )
    flat_query = query_mid.reshape(query_mid.shape[0], query_mid.shape[2])
    pair_cols = pair_mid.shape[2]
    flat_pair = pair_mid.reshape(pair_mid.shape[0], 2 * pair_cols)
    query_full, pair_full = (
        lax.all_gather(flat_query, "replica", axis=0, tiled=True),
        lax.all_gather(flat_pair, "replica", axis=0, tiled=True),
    )
    query_acc = jnp.dot(normed, query_full, preferred_element_type=jnp.float32)
    pair_acc = jnp.dot(normed, pair_full, preferred_element_type=jnp.float32)
    query_local = query_acc.astype(jnp.bfloat16)
    pair_local = pair_acc.astype(jnp.bfloat16).reshape(batch, 2, pair_cols)
    query_heads, pair_heads = (
        lax.all_gather(query_local, "tp", axis=1, tiled=True),
        lax.all_gather(pair_local, "tp", axis=2, tiled=True),
    )
    head_size = key_cache.shape[2]
    kv_heads = pair_heads.shape[2] // head_size
    group = query_heads.shape[1] // (kv_heads * head_size)
    rows_here = key_cache.shape[0]
    first_row = tp_index * rows_here
    query_grouped = (
        query_heads.reshape(batch, kv_heads, group, head_size)
        .transpose(1, 0, 2, 3)
        .reshape(kv_heads * batch, group, head_size)
    )
    key_grouped = (
        pair_heads[:, 0]
        .reshape(batch, kv_heads, head_size)
        .transpose(1, 0, 2)
        .reshape(kv_heads * batch, head_size)
    )
    value_grouped = (
        pair_heads[:, 1]
        .reshape(batch, kv_heads, head_size)
        .transpose(1, 0, 2)
        .reshape(kv_heads * batch, head_size)
    )
    query_mine = lax.dynamic_slice_in_dim(query_grouped, first_row, rows_here, 0)
    key_mine = lax.dynamic_slice_in_dim(key_grouped, first_row, rows_here, 0)
    value_mine = lax.dynamic_slice_in_dim(value_grouped, first_row, rows_here, 0)
    sequence = (first_row + lax.broadcasted_iota(jnp.int32, (rows_here,), 0)) % batch
    matches = sequence[:, None] == lax.broadcasted_iota(jnp.int32, (rows_here, batch), 1)
    row_lengths = jnp.sum(jnp.where(matches, cache_lengths[None, :], 0), axis=1)
    context = attend(query_mine, key_cache, value_cache, key_mine, value_mine, row_lengths)
    context = context.reshape(rows_here, group * head_size)
    return (context, query_full, pair_full.reshape(width, 2, pair_cols))


MESH = pl.DeviceIdType.MESH


def exchange_kernel(
    planes,
    cuts,
    token_in,
    gain_in,
    length_in,
    table_in,
    query_in,
    pair_in,
    key_in,
    value_in,
    query_out,
    pair_out,
    key_out,
    value_out,
    length_out,
    normed_ref,
    spread_ref,
    query_acc,
    token_hold,
    gain_hold,
    gain_wide,
    length_hold,
    table_hold,
    onehot_ref,
    part_ref,
    given,
    joined,
    sums,
    brought,
    pieces,
    send_sem,
    recv_sem,
    hand_recv,
    across_sem,
    local_sem,
    give_send,
    give_recv,
    sum_send,
    sum_recv,
    piece_send,
    piece_recv,
    corner_sem,
):
    r, t = lax.axis_index("replica"), lax.axis_index("tp")
    replicas = 2 * planes
    z, k = r // 2, lax.rem(r, 2)
    ty, tx = t // 2, lax.rem(t, 2)
    rows, query_cols = query_in.shape[0], query_out.shape[1]
    pair_cols = pair_out.shape[2]
    finest = max(cuts.values())
    batch, feats = pieces.shape[1], pieces.shape[2]
    other = [t, ty * 2 + 1 - tx, (1 - ty) * 2 + tx, 3 - t]
    partner = z * 2 + 1 - k

    def piece_id(plane, core, tp):
        return (plane * 2 + core) * 4 + tp

    def part_of(ref, pid, s, cut):
        sub = rows // cut
        return ref.at[pl.ds(pl.multiple_of(pid * rows + s * sub, sub), sub)]

    def slot(pid):
        return (pid // 8) * 4 + lax.rem(pid, 4)

    mine = piece_id(z, k, t)

    def columns(tp, first, count):
        return (
            query_in.at[
                pl.ds(first, count), pl.ds(pl.multiple_of(tp * query_cols, query_cols), query_cols)
            ],
            pair_in.at[
                pl.ds(first, count), :, pl.ds(pl.multiple_of(tp * pair_cols, pair_cols), pair_cols)
            ],
        )

    own = columns(t, 0, rows)
    where_own = pl.ds(pl.multiple_of(mine * rows, rows), rows)
    bring = [
        pltpu.make_async_copy(own[0], query_out.at[where_own], local_sem.at[0]),
        pltpu.make_async_copy(own[1], pair_out.at[where_own], local_sem.at[1]),
    ]
    fetch = [
        pltpu.make_async_copy(token_in, token_hold, local_sem.at[2]),
        pltpu.make_async_copy(table_in, table_hold, local_sem.at[3]),
        pltpu.make_async_copy(gain_in, gain_hold, local_sem.at[4]),
        pltpu.make_async_copy(length_in, length_hold, local_sem.at[5]),
        pltpu.make_async_copy(key_in, key_out, local_sem.at[6]),
        pltpu.make_async_copy(value_in, value_out, local_sem.at[7]),
    ]
    for copy in bring:
        copy.start()

    barrier = pltpu.get_barrier_semaphore()
    for j in range(1, 3):
        pl.semaphore_signal(barrier, inc=1, device_id=(r, other[j]), device_id_type=MESH)
    pl.semaphore_signal(barrier, inc=1, device_id=(partner, t), device_id_type=MESH)
    above, below = lax.rem(r + 2, replicas), lax.rem(r + replicas - 2, replicas)

    @pl.when(z < planes - 1)
    def _():
        pl.semaphore_signal(barrier, inc=1, device_id=(above, t), device_id_type=MESH)

    @pl.when(z > 0)
    def _():
        pl.semaphore_signal(barrier, inc=1, device_id=(below, t), device_id_type=MESH)

    for copy in fetch[:2]:
        copy.start()
    pl.semaphore_wait(barrier, 3 + jnp.minimum(z, 1) + jnp.minimum(planes - 1 - z, 1))

    held = (query_out, pair_out)

    def landed(c, pid, s, cut):
        place = part_of(held[c], pid, s, cut)
        pltpu.make_async_copy(place, place, recv_sem.at[c, slot(pid) * finest + s]).wait()

    def send(c, pid, s, cut, way, target):
        place = part_of(held[c], pid, s, cut)
        pltpu.make_async_remote_copy(
            src_ref=place,
            dst_ref=place,
            send_sem=send_sem.at[c, way],
            recv_sem=(
                hand_recv.at[slot(pid)] if way == 2 else recv_sem.at[c, slot(pid) * finest + s]
            ),
            device_id=target,
            device_id_type=MESH,
        ).start()

    def sent(way, pieces_sent):
        for c, out in enumerate(held):
            place = out.at[0 : pieces_sent * rows]
            pltpu.make_async_copy(place, place, send_sem.at[c, way]).wait()

    def handed(pid):
        place = query_out.at[0 : rows + 2 * rows * pair_cols // query_cols]
        pltpu.make_async_copy(place, place, hand_recv.at[slot(pid)]).wait()

    def across(j):
        cut = cuts["across", j]
        sub = rows // cut

        def act(s, carry):
            sources = columns(other[j], pl.multiple_of(s * sub, sub), sub)
            for c, source in enumerate(sources):
                pltpu.make_async_remote_copy(
                    src_ref=source,
                    dst_ref=part_of(held[c], mine, s, cut),
                    send_sem=across_sem.at[c],
                    recv_sem=recv_sem.at[c, slot(mine) * finest + s],
                    device_id=(r, other[j]),
                    device_id_type=MESH,
                ).start()
            return carry

        lax.fori_loop(0, cut, act, 0)

    def forward(pid, came_in, go_out, up, down):
        groups = min(came_in, go_out) if came_in else go_out

        def act(g, carry):
            for c in range(2):
                for i in range(came_in // groups):
                    landed(c, pid, g * (came_in // groups) + i, came_in)
                for i in range(go_out // groups):
                    s = g * (go_out // groups) + i
                    if up:

                        @pl.when(z < planes - 1)
                        def _():
                            send(c, pid, s, go_out, 0, (above, t))

                    if down:

                        @pl.when(z > 0)
                        def _():
                            send(c, pid, s, go_out, 1, (below, t))

                send(c, pid, g, groups, 2, (partner, t))
            return carry

        lax.fori_loop(0, groups, act, 0)

    def out_cut(far, j):
        return cuts.get((far, j), 1)

    def near(j):
        came_in = cuts["across", j] if j else 0
        forward(piece_id(z, k, other[j]), came_in, out_cut(0, j), True, True)

    def planes_at(far, act):
        if far == 0:
            act(z, True)
            return

        @pl.when(z >= far)
        def _():
            act(lax.rem(z + planes - far, planes), True)

        @pl.when(z + far < planes)
        def _():
            act(lax.rem(z + far, planes), False)

    def far_away(far, j):
        def act(plane, up):
            pid = piece_id(plane, k, other[j])
            forward(pid, out_cut(far - 1, j), out_cut(far, j), up, not up)

        planes_at(far, act)

    def multiply(far, j):
        def both(plane, up):
            def add(turn, carry):
                pid = piece_id(plane, jnp.where(turn == 0, k, 1 - k), other[j])

                @pl.when(turn == 1)
                def _():
                    handed(pid)

                where = pl.ds(pl.multiple_of(pid * rows, rows), rows)
                query_acc[...] += jnp.dot(
                    normed_ref[:, where], query_out[where, :], preferred_element_type=jnp.float32
                )
                return carry

            lax.fori_loop(0, 2, add, 0)

        planes_at(far, both)

    for copy in bring:
        copy.wait()

    near(0)
    pl.semaphore_signal(corner_sem, inc=1, device_id=(r, other[1]), device_id_type=MESH)
    across(1)
    across(2)
    for copy in fetch[2:]:
        copy.start()
    pl.semaphore_wait(corner_sem, 1)
    across(3)

    give = pltpu.make_async_remote_copy(
        src_ref=part_ref.at[:, 1 - k],
        dst_ref=given,
        send_sem=give_send,
        recv_sem=give_recv,
        device_id=(partner, t),
        device_id_type=MESH,
    )

    last = planes - 1

    def passing(hop, wait=False):
        for way in range(2):
            for plane in range(planes - 1):
                if plane != hop and not wait:
                    continue
                place = plane if way == 0 else last - plane
                target = (place + 1 if way == 0 else place - 1) * 2 + k
                dests = range(place + 1, planes) if way == 0 else range(place)

                @pl.when(z == place)
                def _():
                    for dest in dests:
                        if plane > 0 and not wait:
                            came(way, dest)
                            total = joined[dest].astype(jnp.float32) + brought[
                                way, dest
                            ].astype(jnp.float32)
                            sums[way, dest] = total.astype(jnp.bfloat16)
                        copy = pltpu.make_async_remote_copy(
                            src_ref=sums.at[way, dest] if plane > 0 else joined.at[dest],
                            dst_ref=brought.at[way, dest],
                            send_sem=sum_send.at[way, dest],
                            recv_sem=sum_recv.at[way, dest],
                            device_id=(target, t),
                            device_id_type=MESH,
                        )
                        copy.wait_send() if wait else copy.start()

    def came(way, dest):
        place = brought.at[way, dest]
        pltpu.make_async_copy(place, place, sum_recv.at[way, dest]).wait()

    gather = [
        pltpu.make_async_remote_copy(
            src_ref=pieces.at[t],
            dst_ref=pieces.at[t],
            send_sem=piece_send.at[j - 1],
            recv_sem=piece_recv.at[j - 1],
            device_id=(r, other[j]),
            device_id_type=MESH,
        )
        for j in range(1, 4)
    ]

    def select_rows():
        fetch[0].wait()
        vocab_rows = table_hold.shape[0]
        tokens = token_hold.shape[1]
        lanes = 128
        wanted = jnp.broadcast_to(token_hold[...] - r * vocab_rows, (lanes, tokens)).T
        lane = lax.broadcasted_iota(jnp.int32, (tokens, lanes), 1)
        for first in range(0, vocab_rows, lanes):
            onehot_ref[:, first : first + lanes] = (wanted == lane + first).astype(
                onehot_ref.dtype
            )
        fetch[1].wait()
        block = 256

        def select(i, carry):
            where = pl.ds(pl.multiple_of(i * block, block), block)
            rows_here = jnp.dot(
                onehot_ref[...], table_hold[:, where], preferred_element_type=jnp.float32
            ).astype(jnp.bfloat16)
            part_ref[:, :, :, where] = rows_here.reshape(planes, 2, batch, block)
            return carry

        lax.fori_loop(0, feats // block, select, 0)

    def join():
        give.wait()
        for plane in range(planes):
            kept = part_ref[plane, k].astype(jnp.float32)
            joined[plane] = (kept + given[plane].astype(jnp.float32)).astype(jnp.bfloat16)

    def sum_all():
        for dest in range(planes):

            @pl.when(z == dest)
            def _():
                total = joined[dest].astype(jnp.float32)
                for way in range(2):
                    if dest != (0 if way == 0 else last):
                        came(way, dest)
                        total = total + brought[way, dest].astype(jnp.float32)
                pieces[t] = total.astype(jnp.bfloat16)

    def normalise():
        fetch[2].wait()
        gain_wide[...] = gain_hold[...].astype(jnp.float32)
        for copy in gather:
            copy.wait()
        square = jnp.zeros((batch, 1), jnp.float32)
        for i in range(4):
            part = pieces[i].astype(jnp.float32)
            square = square + jnp.sum(part * part, axis=1, keepdims=True)
        factor = lax.rsqrt(square / (4 * feats) + 1e-05)
        lanes = gain_wide.shape[1]
        blocks = feats // lanes
        for i in range(4):

            def scaled(b, carry):
                part = pieces[i, :, pl.ds(pl.multiple_of(b * lanes, lanes), lanes)]
                gain = gain_wide[pl.ds(i * blocks + b, 1), :]
                where = pl.ds(pl.multiple_of(i * feats + b * lanes, lanes), lanes)
                normed_ref[:, where] = (part.astype(jnp.float32) * factor * gain).astype(
                    jnp.bfloat16
                )
                return carry

            lax.fori_loop(0, blocks, scaled, 0)
        block = 256
        line = lax.broadcasted_iota(jnp.int32, (block, 2 * block), 0)
        column = lax.broadcasted_iota(jnp.int32, (block, 2 * block), 1)
        even = (column == 2 * line).astype(jnp.bfloat16)
        odd = (column == 2 * line + 1).astype(jnp.bfloat16)

        def spread(i, carry):
            part = normed_ref[:, pl.ds(pl.multiple_of(i * block, block), block)]
            where = pl.ds(pl.multiple_of(i * 2 * block, 2 * block), 2 * block)
            spread_ref[0:batch, where] = jnp.dot(
                part, even, preferred_element_type=jnp.float32
            ).astype(jnp.bfloat16)
            spread_ref[batch : 2 * batch, where] = jnp.dot(
                part, odd, preferred_element_type=jnp.float32
            ).astype(jnp.bfloat16)
            return carry

        lax.fori_loop(0, 4 * feats // block, spread, 0)

    def lengths():
        fetch[3].wait()
        group = length_out.shape[1]
        for s in range(batch):
            length_out[s] = jnp.full((group, length_out.shape[2]), length_hold[s], jnp.int32)

    select_rows()
    give.start()
    join()
    passing(0)
    order = [(0, 1), (0, 2), (1, 0), (0, 3)]
    order += [(far, j) for far in range(1, planes) for j in range(4) if (far, j) != (1, 0)]
    middle = len(order) - 5
    for step, (far, j) in enumerate(order):
        near(j) if far == 0 else far_away(far, j)
        if step == 1:
            passing(1)
        if step > 4 and step - 3 < planes - 1:
            passing(step - 3)
        if step == middle - 1:
            sum_all()
            for copy in gather:
                copy.start()
        if step == middle:
            normalise()
            lengths()
            query_acc[...] = jnp.zeros_like(query_acc)
            for past in [(0, 0)] + order[:middle]:
                multiply(*past)
        if step > middle:
            multiply(*order[step - 1])

    for copy in fetch[4:]:
        copy.wait()
    for c, out in enumerate((query_out, pair_out)):
        place = out.at[0 : 3 * rows]
        pltpu.make_async_copy(place, place, across_sem.at[c]).wait()
    passing(0, wait=True)
    multiply(*order[-1])
    for place in range(planes):

        @pl.when(z == place)
        def _():
            if place < last:
                sent(0, 4 * (place + 1))
            if place > 0:
                sent(1, 4 * (planes - place))

    sent(2, 4 * planes)


def exchange(
    token_ids, norm_gain, embed_table, w_query, w_keyvalue, key_cache, value_cache, lengths, planes
):
    rows, all_query = w_query.shape
    query_cols, pair_cols = all_query // 4, w_keyvalue.shape[2] // 4
    replicas = 2 * planes
    width = rows * replicas * 4
    feats = embed_table.shape[1]
    kind = w_query.dtype
    batch, head_size = lengths.shape[0], key_cache.shape[2]
    group = query_cols // head_size
    tokens = token_ids.shape[0]
    lanes = 128
    cuts = {("across", 1): 1, ("across", 2): 1, ("across", 3): 1}
    cuts |= {(0, 0): 1, (0, 1): 1, (0, 2): 1, (0, 3): 1}
    anywhere = pl.BlockSpec(memory_space=pl.ANY)
    vmem = pl.BlockSpec(memory_space=pltpu.VMEM)
    dma = pltpu.SemaphoreType.DMA
    shape = jax.ShapeDtypeStruct
    return pl.pallas_call(
        functools.partial(exchange_kernel, planes, cuts),
        out_shape=(
            pltpu.VMEM((width, query_cols), kind),
            pltpu.VMEM((width, 2, pair_cols), kind),
            pltpu.VMEM(key_cache.shape, kind),
            pltpu.VMEM(value_cache.shape, kind),
            pltpu.VMEM((batch, group, head_size), jnp.int32),
            pltpu.VMEM((batch, width), kind),
            pltpu.VMEM((2 * batch, 2 * width), kind),
            pltpu.VMEM((batch, query_cols), jnp.float32),
        ),
        in_specs=[anywhere] * 8,
        out_specs=(vmem,) * 8,
        scratch_shapes=[
            pltpu.VMEM((1, tokens), jnp.int32),
            pltpu.VMEM((width // lanes, lanes), kind),
            pltpu.VMEM((width // lanes, lanes), jnp.float32),
            pltpu.SMEM((batch,), jnp.int32),
            pltpu.VMEM(embed_table.shape, kind),
            pltpu.VMEM((tokens, embed_table.shape[0]), kind),
            pltpu.VMEM((planes, 2, batch, feats), kind),
            pltpu.VMEM((planes, batch, feats), kind),
            pltpu.VMEM((planes, batch, feats), kind),
            pltpu.VMEM((2, planes, batch, feats), kind),
            pltpu.VMEM((2, planes, batch, feats), kind),
            pltpu.VMEM((4, batch, feats), kind),
            dma((2, 3)),
            dma((2, replicas * 2 * max(cuts.values()))),
            dma((replicas * 2,)),
            dma((2,)),
            dma((8,)),
            dma(()),
            dma(()),
            dma((2, planes)),
            dma((2, planes)),
            dma((3,)),
            dma((3,)),
            pltpu.SemaphoreType.REGULAR,
        ],
        compiler_params=pltpu.CompilerParams(
            collective_id=0, has_side_effects=True, vmem_limit_bytes=8 * 2**20
        ),
        cost_estimate=pl.CostEstimate(
            flops=2 * 10**11, bytes_accessed=2 * width * query_cols, transcendentals=0
        ),
        name="weight_exchange",
    )(
        *(
            pltpu.with_memory_space_constraint(operand, pltpu.HBM)
            for operand in (
                token_ids.reshape(1, tokens),
                norm_gain.reshape(-1, lanes),
                lengths,
                embed_table,
                w_query,
                w_keyvalue,
                key_cache,
                value_cache,
            )
        )
    )


def finish_kernel(
    query_acc,
    spread_ref,
    query_all,
    pair_all,
    key_ref,
    value_ref,
    length_ref,
    query_ref,
    pair_ref,
    context_ref,
    query_heads,
    scores_ref,
    weights_ref,
    context_heads,
    context_hold,
    sems,
    context_sem,
):
    pair_cols = pair_all.shape[1]
    batch, group, head_size = query_heads.shape
    parts = sems.shape[1]
    stores = []
    for c, (held, out) in enumerate(((query_all, query_ref), (pair_all, pair_ref))):
        size = held.shape[0] // parts
        for i in range(parts):
            where = pl.ds(i * size, size)
            stores.append(pltpu.make_async_copy(held.at[where], out.at[where], sems.at[c, i]))
    for copy in stores:
        copy.start()

    query = query_acc[...].astype(jnp.bfloat16).astype(jnp.float32)
    for j in range(group):
        query_heads[:, j, :] = query[:, j * head_size : (j + 1) * head_size]
    for s in range(batch):
        scores_ref[s] = lax.dot_general(
            query_heads[s].astype(jnp.bfloat16),
            key_ref[s],
            (((1,), (1,)), ((), ())),
            preferred_element_type=jnp.float32,
        )

    block = 2048

    def project(i, pair):
        here = pl.ds(pl.multiple_of(i * block, block), block)
        return pair + jnp.dot(
            spread_ref[:, here], pair_all[here, :], preferred_element_type=jnp.float32
        )

    pair = lax.fori_loop(
        0,
        pair_all.shape[0] // block,
        project,
        jnp.zeros((2 * batch, pair_cols), jnp.float32),
    )
    pair = pair.astype(jnp.bfloat16).astype(jnp.float32)

    scale = head_size ** (-0.5)
    slots = key_ref.shape[1]
    position = lax.broadcasted_iota(jnp.int32, (group, slots), 1)
    own_weights = []
    for s in range(batch):
        scores = jnp.where(position < length_ref[s, :, 0:1], scores_ref[s] * scale, -jnp.inf)
        own = jnp.sum(query_heads[s] * pair[s : s + 1], axis=1, keepdims=True) * scale
        top = jnp.maximum(jnp.max(scores, axis=1, keepdims=True), own)
        weights = jnp.exp(scores - top)
        own_weight = jnp.exp(own - top)
        share = 1.0 / (jnp.sum(weights, axis=1, keepdims=True) + own_weight)
        weights_ref[s] = (weights * share).astype(jnp.bfloat16)
        own_weights.append((own_weight * share).astype(jnp.bfloat16).astype(jnp.float32))
    for s in range(batch):
        context_heads[s] = (
            jnp.dot(weights_ref[s], value_ref[s], preferred_element_type=jnp.float32)
            + own_weights[s] * pair[batch + s : batch + s + 1]
        )
    for j in range(group):
        context_hold[:, j * head_size : (j + 1) * head_size] = context_heads[:, j, :].astype(
            context_hold.dtype
        )
    context = pltpu.make_async_copy(context_hold, context_ref, context_sem)
    context.start()
    for copy in stores:
        copy.wait()
    context.wait()


def finish(query_acc, spread, query_all, pair_all, keys, values, lengths):
    batch, query_cols = query_acc.shape
    width, _, pair_cols = pair_all.shape
    kind = query_all.dtype
    slots, head_size = keys.shape[1], keys.shape[2]
    group = query_cols // head_size
    pair_flat = pair_all.reshape(2 * width, pair_cols)
    vmem = pl.BlockSpec(memory_space=pltpu.VMEM)
    shape = jax.ShapeDtypeStruct
    query_out, pair_out, context = pl.pallas_call(
        finish_kernel,
        out_shape=(
            shape(query_all.shape, kind),
            shape(pair_flat.shape, kind),
            shape((batch, query_cols), kind),
        ),
        in_specs=[vmem] * 7,
        out_specs=(pl.BlockSpec(memory_space=pltpu.HBM),) * 3,
        scratch_shapes=[
            pltpu.VMEM((batch, group, head_size), jnp.float32),
            pltpu.VMEM((batch, group, slots), jnp.float32),
            pltpu.VMEM((batch, group, slots), kind),
            pltpu.VMEM((batch, group, head_size), jnp.float32),
            pltpu.VMEM((batch, query_cols), kind),
            pltpu.SemaphoreType.DMA((2, 4)),
            pltpu.SemaphoreType.DMA(()),
        ],
        compiler_params=pltpu.CompilerParams(vmem_limit_bytes=8 * 2**20),
        cost_estimate=pl.CostEstimate(
            flops=8 * batch * width * pair_cols,
            bytes_accessed=4 * width * (query_cols + 2 * pair_cols),
            transcendentals=0,
        ),
        name="attend_and_store",
    )(query_acc, spread, query_all, pair_flat, keys, values, lengths)
    return context, query_out, pair_out.reshape(width, 2, pair_cols)


def per_device_line(
    planes,
    token_ids,
    embed_table,
    norm_gain,
    w_query,
    w_keyvalue,
    key_cache,
    value_cache,
    cache_lengths,
):
    query_all, pair_all, keys, values, lengths, _, spread, query_acc = exchange(
        token_ids,
        norm_gain,
        embed_table,
        w_query,
        w_keyvalue,
        key_cache,
        value_cache,
        cache_lengths,
        planes,
    )
    return finish(query_acc, spread, query_all, pair_all, keys, values, lengths)


def solution(mesh):
    replicas, tp = mesh.shape["replica"], mesh.shape["tp"]

    def body(*args):
        key_cache, lengths, w_keyvalue = args[5], args[7], args[4]
        one_head = w_keyvalue.shape[2] == tp * key_cache.shape[2]
        own_rows = key_cache.shape[0] == lengths.shape[0]
        if tp == 4 and replicas % 2 == 0 and replicas > 6 and one_head and own_rows:
            return per_device_line(replicas // 2, *args)
        return per_device(*args)

    return jax.shard_map(
        body,
        mesh=mesh,
        in_specs=(
            P(),
            P("replica", "tp"),
            P(),
            P(("replica", "tp"), None),
            P(("replica", "tp"), None, None),
            P(("replica", "tp"), None, None),
            P(("replica", "tp"), None, None),
            P("replica"),
        ),
        out_specs=(P(("replica", "tp"), None), P(None, "tp"), P(None, None, "tp")),
        check_vma=False,
    )
```

```python
import functools

import jax
import jax.numpy as jnp
from jax import lax
from jax.experimental import pallas as pl
from jax.experimental.pallas import tpu as pltpu
from jax.sharding import PartitionSpec as P


def attend(query, keys, values, key_new, value_new, lengths):
    scale = query.shape[-1] ** (-0.5)
    scores = jnp.einsum("rgd,rcd->rgc", query, keys, preferred_element_type=jnp.float32) * scale
    position = lax.broadcasted_iota(jnp.int32, scores.shape, 2)
    scores = jnp.where(position < lengths[:, None, None], scores, -jnp.inf)
    own = jnp.einsum("rgd,rd->rg", query, key_new, preferred_element_type=jnp.float32) * scale
    top = jnp.maximum(jnp.max(scores, axis=2), own)
    weights = jnp.exp(scores - top[:, :, None])
    own_weight = jnp.exp(own - top)
    total = jnp.sum(weights, axis=2) + own_weight
    weights = (weights / total[:, :, None]).astype(jnp.bfloat16)
    own_weight = (own_weight / total).astype(jnp.bfloat16)
    context = jnp.einsum("rgc,rcd->rgd", weights, values, preferred_element_type=jnp.float32)
    context = (
        context
        + own_weight.astype(jnp.float32)[:, :, None] * value_new.astype(jnp.float32)[:, None, :]
    )
    return context.astype(jnp.bfloat16)


def per_device(
    token_ids, embed_table, norm_gain, w_query, w_keyvalue, key_cache, value_cache, cache_lengths
):
    group_index = lax.axis_index("replica")
    tp_index = lax.axis_index("tp")
    vocab_rows, feature_cols = embed_table.shape
    batch = cache_lengths.shape[0]
    first_id = group_index * vocab_rows
    picked = token_ids - first_id
    columns = lax.broadcasted_iota(jnp.int32, (batch * lax.axis_size("replica"), vocab_rows), 1)
    onehot = (picked[:, None] == columns).astype(jnp.bfloat16)
    embedded = lax.psum_scatter(
        jnp.dot(onehot, embed_table, preferred_element_type=jnp.float32),
        "replica",
        scatter_dimension=0,
        tiled=True,
    ).astype(jnp.bfloat16)
    whole = lax.all_gather(embedded, "tp", axis=1, tiled=True)
    values32 = whole.astype(jnp.float32)
    mean_square = jnp.mean(values32 * values32, axis=1, keepdims=True)
    normed = (values32 * lax.rsqrt(mean_square + 1e-05) * norm_gain.astype(jnp.float32)).astype(
        jnp.bfloat16
    )
    width = normed.shape[1]
    query_rows = w_query.reshape(w_query.shape[0], 1, w_query.shape[1])
    query_mid, pair_mid = (
        lax.all_to_all(query_rows, "tp", split_axis=2, concat_axis=0, tiled=True),
        lax.all_to_all(w_keyvalue, "tp", split_axis=2, concat_axis=0, tiled=True),
    )
    flat_query = query_mid.reshape(query_mid.shape[0], query_mid.shape[2])
    pair_cols = pair_mid.shape[2]
    flat_pair = pair_mid.reshape(pair_mid.shape[0], 2 * pair_cols)
    query_full, pair_full = (
        lax.all_gather(flat_query, "replica", axis=0, tiled=True),
        lax.all_gather(flat_pair, "replica", axis=0, tiled=True),
    )
    query_acc = jnp.dot(normed, query_full, preferred_element_type=jnp.float32)
    pair_acc = jnp.dot(normed, pair_full, preferred_element_type=jnp.float32)
    query_local = query_acc.astype(jnp.bfloat16)
    pair_local = pair_acc.astype(jnp.bfloat16).reshape(batch, 2, pair_cols)
    query_heads, pair_heads = (
        lax.all_gather(query_local, "tp", axis=1, tiled=True),
        lax.all_gather(pair_local, "tp", axis=2, tiled=True),
    )
    head_size = key_cache.shape[2]
    kv_heads = pair_heads.shape[2] // head_size
    group = query_heads.shape[1] // (kv_heads * head_size)
    rows_here = key_cache.shape[0]
    first_row = tp_index * rows_here
    query_grouped = (
        query_heads.reshape(batch, kv_heads, group, head_size)
        .transpose(1, 0, 2, 3)
        .reshape(kv_heads * batch, group, head_size)
    )
    key_grouped = (
        pair_heads[:, 0]
        .reshape(batch, kv_heads, head_size)
        .transpose(1, 0, 2)
        .reshape(kv_heads * batch, head_size)
    )
    value_grouped = (
        pair_heads[:, 1]
        .reshape(batch, kv_heads, head_size)
        .transpose(1, 0, 2)
        .reshape(kv_heads * batch, head_size)
    )
    query_mine = lax.dynamic_slice_in_dim(query_grouped, first_row, rows_here, 0)
    key_mine = lax.dynamic_slice_in_dim(key_grouped, first_row, rows_here, 0)
    value_mine = lax.dynamic_slice_in_dim(value_grouped, first_row, rows_here, 0)
    sequence = (first_row + lax.broadcasted_iota(jnp.int32, (rows_here,), 0)) % batch
    matches = sequence[:, None] == lax.broadcasted_iota(jnp.int32, (rows_here, batch), 1)
    row_lengths = jnp.sum(jnp.where(matches, cache_lengths[None, :], 0), axis=1)
    context = attend(query_mine, key_cache, value_cache, key_mine, value_mine, row_lengths)
    context = context.reshape(rows_here, group * head_size)
    return (context, query_full, pair_full.reshape(width, 2, pair_cols))


MESH = pl.DeviceIdType.MESH


def exchange_kernel(
    planes,
    cuts,
    token_in,
    gain_in,
    length_in,
    table_in,
    query_in,
    pair_in,
    key_in,
    value_in,
    query_out,
    pair_out,
    key_out,
    value_out,
    length_out,
    spread_ref,
    query_acc,
    normed_ref,
    token_hold,
    gain_hold,
    gain_wide,
    length_hold,
    table_hold,
    onehot_ref,
    part_ref,
    given,
    joined,
    sums,
    brought,
    pieces,
    send_sem,
    recv_sem,
    hand_recv,
    across_sem,
    local_sem,
    give_send,
    give_recv,
    sum_send,
    sum_recv,
    piece_send,
    piece_recv,
    corner_sem,
):
    r, t = lax.axis_index("replica"), lax.axis_index("tp")
    replicas = 2 * planes
    z, k = r // 2, lax.rem(r, 2)
    ty, tx = t // 2, lax.rem(t, 2)
    rows, query_cols = query_in.shape[0], query_out.shape[1]
    pair_cols = pair_out.shape[2]
    finest = max(cuts.values())
    batch, feats = pieces.shape[1], pieces.shape[2]
    other = [t, ty * 2 + 1 - tx, (1 - ty) * 2 + tx, 3 - t]
    partner = z * 2 + 1 - k

    def piece_id(plane, core, tp):
        return (plane * 2 + core) * 4 + tp

    def part_of(ref, pid, s, cut):
        sub = rows // cut
        return ref.at[pl.ds(pl.multiple_of(pid * rows + s * sub, sub), sub)]

    def slot(pid):
        return (pid // 8) * 4 + lax.rem(pid, 4)

    mine = piece_id(z, k, t)

    def columns(tp, first, count):
        return (
            query_in.at[
                pl.ds(first, count), pl.ds(pl.multiple_of(tp * query_cols, query_cols), query_cols)
            ],
            pair_in.at[
                pl.ds(first, count), :, pl.ds(pl.multiple_of(tp * pair_cols, pair_cols), pair_cols)
            ],
        )

    own = columns(t, 0, rows)
    where_own = pl.ds(pl.multiple_of(mine * rows, rows), rows)
    bring = [
        pltpu.make_async_copy(own[0], query_out.at[where_own], local_sem.at[0]),
        pltpu.make_async_copy(own[1], pair_out.at[where_own], local_sem.at[1]),
    ]
    fetch = [
        pltpu.make_async_copy(token_in, token_hold, local_sem.at[2]),
        pltpu.make_async_copy(table_in, table_hold, local_sem.at[3]),
        pltpu.make_async_copy(gain_in, gain_hold, local_sem.at[4]),
        pltpu.make_async_copy(length_in, length_hold, local_sem.at[5]),
        pltpu.make_async_copy(key_in, key_out, local_sem.at[6]),
        pltpu.make_async_copy(value_in, value_out, local_sem.at[7]),
    ]
    for copy in bring:
        copy.start()

    barrier = pltpu.get_barrier_semaphore()
    for j in range(1, 3):
        pl.semaphore_signal(barrier, inc=1, device_id=(r, other[j]), device_id_type=MESH)
    pl.semaphore_signal(barrier, inc=1, device_id=(partner, t), device_id_type=MESH)
    above, below = lax.rem(r + 2, replicas), lax.rem(r + replicas - 2, replicas)

    @pl.when(z < planes - 1)
    def _():
        pl.semaphore_signal(barrier, inc=1, device_id=(above, t), device_id_type=MESH)

    @pl.when(z > 0)
    def _():
        pl.semaphore_signal(barrier, inc=1, device_id=(below, t), device_id_type=MESH)

    for copy in fetch[:2]:
        copy.start()
    pl.semaphore_wait(barrier, 3 + jnp.minimum(z, 1) + jnp.minimum(planes - 1 - z, 1))

    held = (query_out, pair_out)

    def landed(c, pid, s, cut):
        place = part_of(held[c], pid, s, cut)
        pltpu.make_async_copy(place, place, recv_sem.at[c, slot(pid) * finest + s]).wait()

    def send(c, pid, s, cut, way, target):
        place = part_of(held[c], pid, s, cut)
        pltpu.make_async_remote_copy(
            src_ref=place,
            dst_ref=place,
            send_sem=send_sem.at[c, way],
            recv_sem=(
                hand_recv.at[slot(pid)] if way == 2 else recv_sem.at[c, slot(pid) * finest + s]
            ),
            device_id=target,
            device_id_type=MESH,
        ).start()

    def sent(way, pieces_sent):
        for c, out in enumerate(held):
            place = out.at[0 : pieces_sent * rows]
            pltpu.make_async_copy(place, place, send_sem.at[c, way]).wait()

    def handed(pid):
        place = query_out.at[0 : rows + 2 * rows * pair_cols // query_cols]
        pltpu.make_async_copy(place, place, hand_recv.at[slot(pid)]).wait()

    def across(j):
        cut = cuts["across", j]
        sub = rows // cut

        def act(s, carry):
            sources = columns(other[j], pl.multiple_of(s * sub, sub), sub)
            for c, source in enumerate(sources):
                pltpu.make_async_remote_copy(
                    src_ref=source,
                    dst_ref=part_of(held[c], mine, s, cut),
                    send_sem=across_sem.at[c],
                    recv_sem=recv_sem.at[c, slot(mine) * finest + s],
                    device_id=(r, other[j]),
                    device_id_type=MESH,
                ).start()
            return carry

        lax.fori_loop(0, cut, act, 0)

    def forward(pid, came_in, go_out, up, down):
        groups = min(came_in, go_out) if came_in else go_out

        def act(g, carry):
            for c in range(2):
                for i in range(came_in // groups):
                    landed(c, pid, g * (came_in // groups) + i, came_in)
                for i in range(go_out // groups):
                    s = g * (go_out // groups) + i
                    if up:

                        @pl.when(z < planes - 1)
                        def _():
                            send(c, pid, s, go_out, 0, (above, t))

                    if down:

                        @pl.when(z > 0)
                        def _():
                            send(c, pid, s, go_out, 1, (below, t))

                send(c, pid, g, groups, 2, (partner, t))
            return carry

        lax.fori_loop(0, groups, act, 0)

    def out_cut(far, j):
        return cuts.get((far, j), 1)

    def near(j):
        came_in = cuts["across", j] if j else 0
        forward(piece_id(z, k, other[j]), came_in, out_cut(0, j), True, True)

    def planes_at(far, act):
        if far == 0:
            act(z, True)
            return

        @pl.when(z >= far)
        def _():
            act(lax.rem(z + planes - far, planes), True)

        @pl.when(z + far < planes)
        def _():
            act(lax.rem(z + far, planes), False)

    def far_away(far, j):
        def act(plane, up):
            pid = piece_id(plane, k, other[j])
            forward(pid, out_cut(far - 1, j), out_cut(far, j), up, not up)

        planes_at(far, act)

    def multiply(far, j):
        def both(plane, up):
            def add(turn, carry):
                pid = piece_id(plane, jnp.where(turn == 0, k, 1 - k), other[j])

                @pl.when(turn == 1)
                def _():
                    handed(pid)

                where = pl.ds(pl.multiple_of(pid * rows, rows), rows)
                query_acc[...] += jnp.dot(
                    normed_ref[:, where], query_out[where, :], preferred_element_type=jnp.float32
                )
                return carry

            lax.fori_loop(0, 2, add, 0)

        planes_at(far, both)

    for copy in bring:
        copy.wait()

    near(0)
    pl.semaphore_signal(corner_sem, inc=1, device_id=(r, other[1]), device_id_type=MESH)
    across(1)
    across(2)
    for copy in fetch[2:]:
        copy.start()
    pl.semaphore_wait(corner_sem, 1)
    across(3)

    give = pltpu.make_async_remote_copy(
        src_ref=part_ref.at[:, 1 - k],
        dst_ref=given,
        send_sem=give_send,
        recv_sem=give_recv,
        device_id=(partner, t),
        device_id_type=MESH,
    )

    last = planes - 1

    def passing(hop, wait=False):
        for way in range(2):
            for plane in range(planes - 1):
                if plane != hop and not wait:
                    continue
                place = plane if way == 0 else last - plane
                target = (place + 1 if way == 0 else place - 1) * 2 + k
                dests = range(place + 1, planes) if way == 0 else range(place)

                @pl.when(z == place)
                def _():
                    for dest in dests:
                        if plane > 0 and not wait:
                            came(way, dest)
                            total = joined[dest].astype(jnp.float32) + brought[
                                way, dest
                            ].astype(jnp.float32)
                            sums[way, dest] = total.astype(jnp.bfloat16)
                        copy = pltpu.make_async_remote_copy(
                            src_ref=sums.at[way, dest] if plane > 0 else joined.at[dest],
                            dst_ref=brought.at[way, dest],
                            send_sem=sum_send.at[way, dest],
                            recv_sem=sum_recv.at[way, dest],
                            device_id=(target, t),
                            device_id_type=MESH,
                        )
                        copy.wait_send() if wait else copy.start()

    def came(way, dest):
        place = brought.at[way, dest]
        pltpu.make_async_copy(place, place, sum_recv.at[way, dest]).wait()

    gather = [
        pltpu.make_async_remote_copy(
            src_ref=pieces.at[t],
            dst_ref=pieces.at[t],
            send_sem=piece_send.at[j - 1],
            recv_sem=piece_recv.at[j - 1],
            device_id=(r, other[j]),
            device_id_type=MESH,
        )
        for j in range(1, 4)
    ]

    def select_rows():
        fetch[0].wait()
        vocab_rows = table_hold.shape[0]
        tokens = token_hold.shape[1]
        lanes = 128
        wanted = jnp.broadcast_to(token_hold[...] - r * vocab_rows, (lanes, tokens)).T
        lane = lax.broadcasted_iota(jnp.int32, (tokens, lanes), 1)
        for first in range(0, vocab_rows, lanes):
            onehot_ref[:, first : first + lanes] = (wanted == lane + first).astype(
                onehot_ref.dtype
            )
        fetch[1].wait()
        block = 256

        def select(i, carry):
            where = pl.ds(pl.multiple_of(i * block, block), block)
            rows_here = jnp.dot(
                onehot_ref[...], table_hold[:, where], preferred_element_type=jnp.float32
            ).astype(jnp.bfloat16)
            part_ref[:, :, :, where] = rows_here.reshape(planes, 2, batch, block)
            return carry

        lax.fori_loop(0, feats // block, select, 0)

    def join():
        give.wait()
        for plane in range(planes):
            kept = part_ref[plane, k].astype(jnp.float32)
            joined[plane] = (kept + given[plane].astype(jnp.float32)).astype(jnp.bfloat16)

    def sum_all():
        for dest in range(planes):

            @pl.when(z == dest)
            def _():
                total = joined[dest].astype(jnp.float32)
                for way in range(2):
                    if dest != (0 if way == 0 else last):
                        came(way, dest)
                        total = total + brought[way, dest].astype(jnp.float32)
                pieces[t] = total.astype(jnp.bfloat16)

    def normalise():
        fetch[2].wait()
        gain_wide[...] = gain_hold[...].astype(jnp.float32)
        for copy in gather:
            copy.wait()
        square = jnp.zeros((batch, 1), jnp.float32)
        for i in range(4):
            part = pieces[i].astype(jnp.float32)
            square = square + jnp.sum(part * part, axis=1, keepdims=True)
        factor = lax.rsqrt(square / (4 * feats) + 1e-05)
        lanes = gain_wide.shape[1]
        blocks = feats // lanes
        for i in range(4):

            def scaled(b, carry):
                part = pieces[i, :, pl.ds(pl.multiple_of(b * lanes, lanes), lanes)]
                gain = gain_wide[pl.ds(i * blocks + b, 1), :]
                where = pl.ds(pl.multiple_of(i * feats + b * lanes, lanes), lanes)
                normed_ref[:, where] = (part.astype(jnp.float32) * factor * gain).astype(
                    jnp.bfloat16
                )
                return carry

            lax.fori_loop(0, blocks, scaled, 0)
        block = 256
        line = lax.broadcasted_iota(jnp.int32, (block, 2 * block), 0)
        column = lax.broadcasted_iota(jnp.int32, (block, 2 * block), 1)
        even = (column == 2 * line).astype(jnp.bfloat16)
        odd = (column == 2 * line + 1).astype(jnp.bfloat16)

        def spread(i, carry):
            part = normed_ref[:, pl.ds(pl.multiple_of(i * block, block), block)]
            where = pl.ds(pl.multiple_of(i * 2 * block, 2 * block), 2 * block)
            spread_ref[0:batch, where] = jnp.dot(
                part, even, preferred_element_type=jnp.float32
            ).astype(jnp.bfloat16)
            spread_ref[batch : 2 * batch, where] = jnp.dot(
                part, odd, preferred_element_type=jnp.float32
            ).astype(jnp.bfloat16)
            return carry

        lax.fori_loop(0, 4 * feats // block, spread, 0)

    def lengths():
        fetch[3].wait()
        group = length_out.shape[1]
        for s in range(batch):
            length_out[s] = jnp.full((group, length_out.shape[2]), length_hold[s], jnp.int32)

    select_rows()
    give.start()
    join()
    passing(0)
    order = [(0, 1), (0, 2), (1, 0), (0, 3)]
    order += [(far, j) for far in range(1, planes) for j in range(4) if (far, j) != (1, 0)]
    middle = len(order) - 5
    for step, (far, j) in enumerate(order):
        near(j) if far == 0 else far_away(far, j)
        if step == 1:
            passing(1)
        if step > 4 and step - 3 < planes - 1:
            passing(step - 3)
        if step == middle - 1:
            sum_all()
            for copy in gather:
                copy.start()
        if step == middle:
            normalise()
            lengths()
            query_acc[...] = jnp.zeros_like(query_acc)
            for past in [(0, 0)] + order[:middle]:
                multiply(*past)
        if step > middle:
            multiply(*order[step - 1])

    for copy in fetch[4:]:
        copy.wait()
    for c, out in enumerate((query_out, pair_out)):
        place = out.at[0 : 3 * rows]
        pltpu.make_async_copy(place, place, across_sem.at[c]).wait()
    passing(0, wait=True)
    multiply(*order[-1])
    for place in range(planes):

        @pl.when(z == place)
        def _():
            if place < last:
                sent(0, 4 * (place + 1))
            if place > 0:
                sent(1, 4 * (planes - place))

    sent(2, 4 * planes)


def exchange(
    token_ids, norm_gain, embed_table, w_query, w_keyvalue, key_cache, value_cache, lengths, planes
):
    rows, all_query = w_query.shape
    query_cols, pair_cols = all_query // 4, w_keyvalue.shape[2] // 4
    replicas = 2 * planes
    width = rows * replicas * 4
    feats = embed_table.shape[1]
    kind = w_query.dtype
    batch, head_size = lengths.shape[0], key_cache.shape[2]
    group = query_cols // head_size
    tokens = token_ids.shape[0]
    lanes = 128
    cuts = {("across", 1): 1, ("across", 2): 1, ("across", 3): 1}
    cuts |= {(0, 0): 1, (0, 1): 1, (0, 2): 1, (0, 3): 1}
    anywhere = pl.BlockSpec(memory_space=pl.ANY)
    vmem = pl.BlockSpec(memory_space=pltpu.VMEM)
    dma = pltpu.SemaphoreType.DMA
    shape = jax.ShapeDtypeStruct
    return pl.pallas_call(
        functools.partial(exchange_kernel, planes, cuts),
        out_shape=(
            pltpu.VMEM((width, query_cols), kind),
            pltpu.VMEM((width, 2, pair_cols), kind),
            pltpu.VMEM(key_cache.shape, kind),
            pltpu.VMEM(value_cache.shape, kind),
            pltpu.VMEM((batch, group, head_size), jnp.int32),
            pltpu.VMEM((2 * batch, 2 * width), kind),
            pltpu.VMEM((batch, query_cols), jnp.float32),
        ),
        in_specs=[anywhere] * 8,
        out_specs=(vmem,) * 7,
        scratch_shapes=[
            pltpu.VMEM((batch, width), kind),
            pltpu.VMEM((1, tokens), jnp.int32),
            pltpu.VMEM((width // lanes, lanes), kind),
            pltpu.VMEM((width // lanes, lanes), jnp.float32),
            pltpu.SMEM((batch,), jnp.int32),
            pltpu.VMEM(embed_table.shape, kind),
            pltpu.VMEM((tokens, embed_table.shape[0]), kind),
            pltpu.VMEM((planes, 2, batch, feats), kind),
            pltpu.VMEM((planes, batch, feats), kind),
            pltpu.VMEM((planes, batch, feats), kind),
            pltpu.VMEM((2, planes, batch, feats), kind),
            pltpu.VMEM((2, planes, batch, feats), kind),
            pltpu.VMEM((4, batch, feats), kind),
            dma((2, 3)),
            dma((2, replicas * 2 * max(cuts.values()))),
            dma((replicas * 2,)),
            dma((2,)),
            dma((8,)),
            dma(()),
            dma(()),
            dma((2, planes)),
            dma((2, planes)),
            dma((3,)),
            dma((3,)),
            pltpu.SemaphoreType.REGULAR,
        ],
        compiler_params=pltpu.CompilerParams(
            collective_id=0, has_side_effects=True, vmem_limit_bytes=8 * 2**20
        ),
        cost_estimate=pl.CostEstimate(
            flops=2 * 10**11, bytes_accessed=2 * width * query_cols, transcendentals=0
        ),
        name="weight_exchange",
    )(
        *(
            pltpu.with_memory_space_constraint(operand, pltpu.HBM)
            for operand in (
                token_ids.reshape(1, tokens),
                norm_gain.reshape(-1, lanes),
                lengths,
                embed_table,
                w_query,
                w_keyvalue,
                key_cache,
                value_cache,
            )
        )
    )


def finish_kernel(
    query_acc,
    spread_ref,
    query_all,
    pair_all,
    key_ref,
    value_ref,
    length_ref,
    query_ref,
    pair_ref,
    context_ref,
    query_heads,
    scores_ref,
    weights_ref,
    context_heads,
    context_hold,
    sems,
    context_sem,
):
    pair_cols = pair_all.shape[1]
    batch, group, head_size = query_heads.shape
    parts = sems.shape[1]
    stores = []
    for c, (held, out) in enumerate(((query_all, query_ref), (pair_all, pair_ref))):
        size = held.shape[0] // parts
        for i in range(parts):
            where = pl.ds(i * size, size)
            stores.append(pltpu.make_async_copy(held.at[where], out.at[where], sems.at[c, i]))
    for copy in stores:
        copy.start()

    query = query_acc[...].astype(jnp.bfloat16).astype(jnp.float32)
    for j in range(group):
        query_heads[:, j, :] = query[:, j * head_size : (j + 1) * head_size]
    for s in range(batch):
        scores_ref[s] = lax.dot_general(
            query_heads[s].astype(jnp.bfloat16),
            key_ref[s],
            (((1,), (1,)), ((), ())),
            preferred_element_type=jnp.float32,
        )

    block = 2048

    def project(i, pair):
        here = pl.ds(pl.multiple_of(i * block, block), block)
        return pair + jnp.dot(
            spread_ref[:, here], pair_all[here, :], preferred_element_type=jnp.float32
        )

    pair = lax.fori_loop(
        0,
        pair_all.shape[0] // block,
        project,
        jnp.zeros((2 * batch, pair_cols), jnp.float32),
    )
    pair = pair.astype(jnp.bfloat16).astype(jnp.float32)

    scale = head_size ** (-0.5)
    slots = key_ref.shape[1]
    position = lax.broadcasted_iota(jnp.int32, (group, slots), 1)
    own_weights = []
    for s in range(batch):
        scores = jnp.where(position < length_ref[s, :, 0:1], scores_ref[s] * scale, -jnp.inf)
        own = jnp.sum(query_heads[s] * pair[s : s + 1], axis=1, keepdims=True) * scale
        top = jnp.maximum(jnp.max(scores, axis=1, keepdims=True), own)
        weights = jnp.exp(scores - top)
        own_weight = jnp.exp(own - top)
        share = 1.0 / (jnp.sum(weights, axis=1, keepdims=True) + own_weight)
        weights_ref[s] = (weights * share).astype(jnp.bfloat16)
        own_weights.append((own_weight * share).astype(jnp.bfloat16).astype(jnp.float32))
    for s in range(batch):
        context_heads[s] = (
            jnp.dot(weights_ref[s], value_ref[s], preferred_element_type=jnp.float32)
            + own_weights[s] * pair[batch + s : batch + s + 1]
        )
    for j in range(group):
        context_hold[:, j * head_size : (j + 1) * head_size] = context_heads[:, j, :].astype(
            context_hold.dtype
        )
    context = pltpu.make_async_copy(context_hold, context_ref, context_sem)
    context.start()
    for copy in stores:
        copy.wait()
    context.wait()


def finish(query_acc, spread, query_all, pair_all, keys, values, lengths):
    batch, query_cols = query_acc.shape
    width, _, pair_cols = pair_all.shape
    kind = query_all.dtype
    slots, head_size = keys.shape[1], keys.shape[2]
    group = query_cols // head_size
    pair_flat = pair_all.reshape(2 * width, pair_cols)
    vmem = pl.BlockSpec(memory_space=pltpu.VMEM)
    shape = jax.ShapeDtypeStruct
    query_out, pair_out, context = pl.pallas_call(
        finish_kernel,
        out_shape=(
            shape(query_all.shape, kind),
            shape(pair_flat.shape, kind),
            shape((batch, query_cols), kind),
        ),
        in_specs=[vmem] * 7,
        out_specs=(pl.BlockSpec(memory_space=pltpu.HBM),) * 3,
        scratch_shapes=[
            pltpu.VMEM((batch, group, head_size), jnp.float32),
            pltpu.VMEM((batch, group, slots), jnp.float32),
            pltpu.VMEM((batch, group, slots), kind),
            pltpu.VMEM((batch, group, head_size), jnp.float32),
            pltpu.VMEM((batch, query_cols), kind),
            pltpu.SemaphoreType.DMA((2, 4)),
            pltpu.SemaphoreType.DMA(()),
        ],
        compiler_params=pltpu.CompilerParams(vmem_limit_bytes=8 * 2**20),
        cost_estimate=pl.CostEstimate(
            flops=8 * batch * width * pair_cols,
            bytes_accessed=4 * width * (query_cols + 2 * pair_cols),
            transcendentals=0,
        ),
        name="attend_and_store",
    )(query_acc, spread, query_all, pair_flat, keys, values, lengths)
    return context, query_out, pair_out.reshape(width, 2, pair_cols)


def per_device_line(
    planes,
    token_ids,
    embed_table,
    norm_gain,
    w_query,
    w_keyvalue,
    key_cache,
    value_cache,
    cache_lengths,
):
    query_all, pair_all, keys, values, lengths, spread, query_acc = exchange(
        token_ids,
        norm_gain,
        embed_table,
        w_query,
        w_keyvalue,
        key_cache,
        value_cache,
        cache_lengths,
        planes,
    )
    return finish(query_acc, spread, query_all, pair_all, keys, values, lengths)


def solution(mesh):
    replicas, tp = mesh.shape["replica"], mesh.shape["tp"]

    def body(*args):
        key_cache, lengths, w_keyvalue = args[5], args[7], args[4]
        one_head = w_keyvalue.shape[2] == tp * key_cache.shape[2]
        own_rows = key_cache.shape[0] == lengths.shape[0]
        if tp == 4 and replicas % 2 == 0 and replicas > 6 and one_head and own_rows:
            return per_device_line(replicas // 2, *args)
        return per_device(*args)

    return jax.shard_map(
        body,
        mesh=mesh,
        in_specs=(
            P(),
            P("replica", "tp"),
            P(),
            P(("replica", "tp"), None),
            P(("replica", "tp"), None, None),
            P(("replica", "tp"), None, None),
            P(("replica", "tp"), None, None),
            P("replica"),
        ),
        out_specs=(P(("replica", "tp"), None), P(None, "tp"), P(None, None, "tp")),
        check_vma=False,
    )
```
